32 devices in a mesh: chan: 8 (over z, y), slot: 4 (over x, core).
Axes of the slice: x: 2, y: 2, z: 4, core: 2. Of those that a mesh axis runs over, the one named last changes fastest.
Arguments:
- visibility: float32 [2, 2, 32, 4, 3844], P(None, None, 'chan', 'slot'), parts along dimension 3, may hold values from -6 to 6
- coherency: bfloat16 [2, 2, 16, 32, 4, 3844], P(None, None, None, 'chan', 'slot'), parts along dimension 4, may hold values from -2 to 2
- jones_start: float32 [2, 2, 64, 32, 62], P(None, None, 'slot', 'chan'), parts along dimension 2, may hold values from -4 to 4
- duals_start: float32 [2, 2, 64, 32, 62], P(None, None, 'slot', 'chan'), parts along dimension 2, may hold values from -2 to 2
Outputs:
- jones_final: float32 [2, 2, 64, 32, 62], P(None, None, 'slot', 'chan'), parts along dimension 2
- consensus: float32 [2, 2, 64, 32, 62], P(None, None, 'slot', 'chan'), parts along dimension 2
- duals_final: float32 [2, 2, 64, 32, 62], P(None, None, 'slot', 'chan'), parts along dimension 2
- norms: float32 [8, 2], P('slot'), parts along dimension 0
The draws below stay inside these ranges and needn't reach their ends.
There are 4 independent parts, one for each index of `slot`. The reference program is written for one: setup_inputs(seed, part) draws one part's arguments, and reference() takes and returns one part's arrays. A program takes and returns all parts, laid end to end along the dimension named above; each array names one. Nothing has to cross between parts.
All inputs are finite; a program needn't handle non-finite values.
Results may differ from the reference program's by a relative error of at most 0.0003.
Values sent between devices are 32-bit elements; how exact they have to be, the bound alone decides.
A program may use at most 128 MiB of HBM per device.

```python
import jax
import jax.numpy as jnp
from jax import lax

STATIONS = 62
DIRS = 16
POLS = 2
TIMES = 1
ITERS = 2
CH_DEV = 4
CHANNELS = 32
PAIRS = 3844
N_CHAN = 8


def block_levels(key, extent, cuts, low, high):
    def one(dim, shards_of):
        heights = jax.random.uniform(jax.random.fold_in(jax.random.fold_in(key, 6), dim), (shards_of,), jnp.float32, low / len(cuts), high / len(cuts))
        return jnp.repeat(jnp.exp(heights), extent[dim] // shards_of).reshape((-1,) + (1,) * (len(extent) - dim - 1))

    level = one(*cuts[0])
    for cut in cuts[1:]:
        level = level * one(*cut)
    return level


def scatter_about(rng, dims, scale, bound, split=(), kind=jnp.bfloat16):
    values = jax.random.normal(rng, dims, jnp.float32) * scale
    if len(split) > 0:
        values = block_levels(rng, dims, split, -0.22, 0.18) * values
    return jnp.clip(values, min=-bound, max=bound).astype(kind)


def setup_inputs(seed: int = 0, part: int = 0) -> dict:
    key_list = jax.random.split(jax.random.key(seed), 5)
    part_splits = jax.random.split(jax.random.fold_in(key_list[4], part), 5)
    visibility = scatter_about(part_splits[0], (2, POLS, CHANNELS, TIMES, PAIRS), 1.0, 6.0, ((2, 8),), jnp.float32)
    coherency = scatter_about(part_splits[1], (2, POLS, DIRS, CHANNELS, TIMES, PAIRS), 0.25, 2.0, ((3, 8),))
    jones_start = scatter_about(part_splits[2], (2, POLS, DIRS, CHANNELS, STATIONS), 0.7, 4.0, ((3, 8),), jnp.float32)
    duals_start = scatter_about(part_splits[3], (2, POLS, DIRS, CHANNELS, STATIONS), 0.3, 2.0, ((3, 8),), jnp.float32)
    return {"visibility": visibility, "coherency": coherency, "jones_start": jones_start, "duals_start": duals_start}


penalty = 8.0
kernel_taps = (0.04, 0.06, 0.1, 0.15, 0.3, 0.15, 0.1, 0.06, 0.04)


def jones_update(visibility, coherency, jones_now, target):
    width = jones_now.shape[-1]
    grid_shape = coherency.shape[1:5] + (width, width)
    sky_real = coherency[0].astype(jnp.float32).reshape(grid_shape)
    sky_imag = coherency[1].astype(jnp.float32).reshape(grid_shape)
    vis_shape = visibility.shape[1:4] + (width, width)
    data_real = visibility[0].reshape(vis_shape)[:, None]
    data_imag = visibility[1].reshape(vis_shape)[:, None]
    left_real = jones_now[0][:, :, :, None, :, None]
    left_imag = jones_now[1][:, :, :, None, :, None]
    right_real = jones_now[0][:, :, :, None, None, :]
    right_imag = jones_now[1][:, :, :, None, None, :]
    crossed = 1.0 - jnp.eye(width, dtype=jnp.float32)
    half_real = left_real * sky_real - left_imag * sky_imag
    half_imag = left_real * sky_imag + left_imag * sky_real
    model_real = half_real * right_real + half_imag * right_imag
    model_imag = half_imag * right_real - half_real * right_imag
    rest_real = (data_real - jnp.sum(model_real, axis=1, keepdims=True) + model_real) * crossed
    rest_imag = (data_imag - jnp.sum(model_imag, axis=1, keepdims=True) + model_imag) * crossed
    weight_real = sky_real * right_real + sky_imag * right_imag
    weight_imag = sky_real * right_imag - sky_imag * right_real
    upper_real = jnp.sum(rest_real * weight_real - rest_imag * weight_imag, axis=(3, 5))
    upper_imag = jnp.sum(rest_real * weight_imag + rest_imag * weight_real, axis=(3, 5))
    lower = jnp.sum(crossed * (sky_real * sky_real + sky_imag * sky_imag) * (right_real * right_real + right_imag * right_imag), axis=(3, 5)) + penalty
    return jnp.stack([(upper_real + penalty * target[0]) / lower, (upper_imag + penalty * target[1]) / lower])


def blocked_update(visibility, coherency, jones_now, target):
    vis_shape = visibility.shape
    vis_blocks = jnp.moveaxis(visibility.reshape(vis_shape[:2] + (N_CHAN, CH_DEV) + vis_shape[3:]), 2, 0)
    coh_shape = coherency.shape
    coh_blocks = jnp.moveaxis(coherency.reshape(coh_shape[:3] + (N_CHAN, CH_DEV) + coh_shape[4:]), 3, 0)
    gain_shape = jones_now.shape
    gain_blocks = jnp.moveaxis(jones_now.reshape(gain_shape[:3] + (N_CHAN, CH_DEV) + gain_shape[4:]), 3, 0)
    target_blocks = jnp.moveaxis(target.reshape(gain_shape[:3] + (N_CHAN, CH_DEV) + gain_shape[4:]), 3, 0)
    updated = lax.map(lambda blocks_in: jones_update(*blocks_in), (vis_blocks, coh_blocks, gain_blocks, target_blocks))
    return jnp.moveaxis(updated, 0, 3).reshape(gain_shape)


def smooth(padded, channels):
    total = kernel_taps[0] * padded[:, :, :, 0:channels]
    for offset in range(1, 9):
        total = total + kernel_taps[offset] * padded[:, :, :, offset:offset + channels]
    return total


def reference(visibility, coherency, jones_start, duals_start):
    channels = jones_start.shape[3]
    entries = jones_start.size
    jones_now = jones_start
    consensus = jones_start
    duals_now = duals_start
    partials = []
    for iteration in range(ITERS):
        jones_now = blocked_update(visibility, coherency, jones_now, consensus - duals_now)
        summed = jones_now + duals_now
        padded = jnp.pad(summed, ((0, 0), (0, 0), (0, 0), (4, 4), (0, 0)))
        fresh = smooth(padded, channels)
        duals_now = duals_now + jones_now - fresh
        primal_gap = jones_now - fresh
        moved = fresh - consensus
        primal = jnp.sum(primal_gap * primal_gap) / entries
        change = penalty * penalty * jnp.sum(moved * moved) / entries
        partials.append(jnp.stack([primal, change]))
        consensus = fresh
    return jones_now, consensus, duals_now, jnp.stack(partials)
```

```python
import functools

import jax
import jax.numpy as jnp
from jax import lax
from jax.experimental import pallas as pl
from jax.experimental.pallas import tpu as pltpu
from jax.sharding import PartitionSpec as P

ITERS = 2
PITCH = 64
GROUP = 8
CHUNKS = 2
MESH = pl.DeviceIdType.MESH

penalty = 8.0
kernel_taps = (0.04, 0.06, 0.1, 0.15, 0.3, 0.15, 0.1, 0.06, 0.04)


def kernel(
    count, dims,
    vis_in, sky_in, jones_in, duals_in,
    jones_out, consensus_out, duals_out, norms_out,
    vis_raw, sky_raw, tail_raw, jones_raw, duals_raw,
    vis_rows, base, mixer, sky, vis, z_keep, rest, acc,
    gain, cons, dual, summed, from_low, from_high, sums, slots,
    load_sem, sky_sem, tail_sem, send_sem, low_sem, high_sem, norm_send, norm_recv,
):
    pols, dirs, channels, width, pairs, entries = dims
    lanes = pols * dirs * channels
    tiles = pl.cdiv(pairs, 128)
    whole = pairs // 128
    me = lax.axis_index("chan")

    loads = [
        pltpu.make_async_copy(source, target, load_sem.at[i])
        for i, (source, target) in enumerate(((vis_in, vis_raw), (jones_in, jones_raw), (duals_in, duals_raw)))
    ]
    sky_loads = [
        pltpu.make_async_copy(sky_in.at[:, :, :, :, 128 * j : 128 * j + 128], sky_raw.at[j], sky_sem.at[j])
        for j in range(whole)
    ]
    tail_load = pltpu.make_async_copy(sky_in.at[:, :, :, :, 128 * whole : pairs], tail_raw, tail_sem)
    for copy in loads + sky_loads + [tail_load]:
        copy.start()

    from_low[...] = jnp.zeros_like(from_low)
    from_high[...] = jnp.zeros_like(from_high)
    barrier = pltpu.get_barrier_semaphore()
    for step in range(1, count):
        pl.semaphore_signal(barrier, inc=1, device_id={"chan": lax.rem(me + step, count)}, device_id_type=MESH)

    sums[...] = jnp.zeros_like(sums)
    sky_raw[whole] = jnp.zeros(sky_raw.shape[1:], sky_raw.dtype)
    sky[:, width:] = jnp.zeros((2, PITCH - width, PITCH, lanes), jnp.float32)
    vis[:, width:] = jnp.zeros((2, PITCH - width, PITCH, lanes), jnp.float32)
    vis_rows[:, :, 128 * whole :] = jnp.zeros((2, 2 * channels, 128 * (tiles - whole)), jnp.float32)
    row = lax.broadcasted_iota(jnp.int32, (2 * PITCH, 256), 0)
    col = lax.broadcasted_iota(jnp.int32, (2 * PITCH, 256), 1)
    station = row & (PITCH - 1)
    target = jnp.where(row >= PITCH, station + width, station)
    base[...] = jnp.where(station < width, col - target, -1024)
    row = lax.broadcasted_iota(jnp.int32, (2 * lanes, lanes), 0) & (lanes - 1)
    col = lax.broadcasted_iota(jnp.int32, (2 * lanes, lanes), 1)
    half = dirs * channels
    same = ((row >= half) == (col >= half)) & ((row & (channels - 1)) == (col & (channels - 1)))
    mixer[...] = jnp.where(same, -1.0, 0.0).astype(jnp.bfloat16)

    def chooser(i):
        return jnp.where(base[...] == (2 * width * i) % 128, 1.0, 0.0).astype(jnp.bfloat16)

    def swung(left, right):
        return lax.dot_general(left, right, (((1,), (1,)), ((), ())), preferred_element_type=jnp.float32)

    loads[0].wait()
    for part in range(2):
        for pol in range(pols):
            for f in range(channels):
                vis_rows[part, pol * channels + f : pol * channels + f + 1, 0:pairs] = vis_raw[part, pol, f]
    upper = lax.broadcasted_iota(jnp.int32, (2 * channels, 256), 0) < channels
    lane = lax.broadcasted_iota(jnp.int32, (2 * PITCH, lanes), 1)
    real = (lane & 8) == 0
    gap = jnp.zeros((half - 16, 256), jnp.float32)
    for i in range(width // 2):
        j = (2 * width * i) // 128
        first, second = [], []
        for part in range(2):
            value = vis_rows[part, :, 128 * j : 128 * j + 256]
            high = value.astype(jnp.bfloat16).astype(jnp.float32)
            low = pltpu.roll(value - high, channels, 0)
            first.append(jnp.where(upper, high, low))
            second.append(jnp.where(upper, low, high))
        right = jnp.concatenate(first + [gap] + second + [gap], 0).astype(jnp.bfloat16)
        turned = swung(chooser(i), right)
        vis[0, 2 * i : 2 * i + 2] = jnp.where(real, turned, 0.0).reshape(2, PITCH, lanes)
        vis[1, 2 * i : 2 * i + 2] = jnp.where(real, 0.0, turned).reshape(2, PITCH, lanes)

    for copy in loads[1:]:
        copy.wait()
    for part in range(2):
        start = jnp.transpose(jones_raw[part].reshape(lanes, width))
        gain[0, part, 0:width] = start
        cons[part, 0:width] = start
        dual[part, 0:width] = jnp.transpose(duals_raw[part].reshape(lanes, width))
        empty = jnp.zeros((PITCH - width, lanes), jnp.float32)
        gain[0, part, width:] = empty
        cons[part, width:] = empty
        dual[part, width:] = empty

    for j in range(whole):
        sky_loads[j].wait()
    tail_load.wait()
    sky_raw[whole, :, :, :, :, 0 : pairs - 128 * whole] = tail_raw[...]
    for i in range(width // 2):
        j = (2 * width * i) // 128
        right = jnp.concatenate(
            [sky_raw[j].reshape(2 * lanes, 128), sky_raw[j + 1].reshape(2 * lanes, 128)], 1
        )
        turned = swung(chooser(i), right)
        for part in range(2):
            sky[part, 2 * i : 2 * i + 2] = turned[:, part * lanes : (part + 1) * lanes].reshape(2, PITCH, lanes)
            for p in (2 * i, 2 * i + 1):
                sky[part, p, p : p + 1] = jnp.zeros((1, lanes), jnp.float32)

    def parted(value):
        high = value.astype(jnp.bfloat16)
        low = (value - high.astype(jnp.float32)).astype(jnp.bfloat16)
        return jnp.concatenate([high, low], 1)

    def sweep(it, block, carry):
        gr, gi = gain[it, 0], gain[it, 1]
        sides = ([], [])
        for b in range(GROUP):
            p = block * GROUP + b
            sr, si = sky[0, p], sky[1, p]
            zr = sr * gr + si * gi
            zi = sr * gi - si * gr
            z_keep[0, b] = zr
            z_keep[1, b] = zi
            lr, li = gain[it, 0, pl.ds(p, 1)], gain[it, 1, pl.ds(p, 1)]
            sides[0].append(parted(lr * zr + li * zi - vis[0, p]))
            sides[1].append(parted(li * zr - lr * zi - vis[1, p]))
        for part in range(2):
            rest[part] = jnp.dot(
                jnp.concatenate(sides[part], 0), mixer[...], preferred_element_type=jnp.float32
            ).reshape(GROUP, PITCH, lanes)
        sums_of = ([], [], [])
        for b in range(GROUP):
            zr, zi = z_keep[0, b], z_keep[1, b]
            dr, di = rest[0, b], rest[1, b]
            for i, value in enumerate((dr * zr - di * zi, dr * zi + di * zr, zr * zr + zi * zi)):
                sums_of[i].append(jnp.sum(value, 0, keepdims=True))
        for i in range(3):
            acc[i, pl.ds(pl.multiple_of(block * GROUP, GROUP), GROUP)] = jnp.concatenate(sums_of[i], 0)
        return carry

    tall = PITCH // CHUNKS
    place = lax.broadcasted_iota(jnp.int32, (tall, lanes), 1) & (channels - 1)

    def mixed(block, distance):
        out = None
        for shift in range(1 - channels, channels):
            offset = distance + shift + 4
            if offset < 0 or offset > 8:
                continue
            inside = (place + shift >= 0) & (place + shift < channels)
            weight = jnp.where(inside, kernel_taps[offset], 0.0)
            moved = block if shift == 0 else pltpu.roll(block, (-shift) % lanes, 1)
            term = weight * moved
            out = term if out is None else out + term
        return out

    def up_copy(it, chunk):
        return pltpu.make_async_remote_copy(
            src_ref=summed.at[it, chunk], dst_ref=from_low.at[it, chunk],
            send_sem=send_sem.at[it, chunk, 0], recv_sem=low_sem.at[it, chunk],
            device_id={"chan": lax.rem(me + 1, count)}, device_id_type=MESH,
        )

    def down_copy(it, chunk):
        return pltpu.make_async_remote_copy(
            src_ref=summed.at[it, chunk], dst_ref=from_high.at[it, chunk],
            send_sem=send_sem.at[it, chunk, 1], recv_sem=high_sem.at[it, chunk],
            device_id={"chan": lax.rem(me + count - 1, count)}, device_id_type=MESH,
        )

    def finish(it, chunk):
        rows = slice(chunk * tall, (chunk + 1) * tall)
        lower = acc[2, rows]
        scale = lower + penalty
        for part in range(2):
            goal = cons[part, rows] - dual[part, rows]
            fresh = (acc[part, rows] + gain[it, part, rows] * lower + penalty * goal) / scale
            gain[it + 1, part, rows] = fresh
            summed[it, chunk, part] = fresh + dual[part, rows]

        @pl.when(me < count - 1)
        def _():
            up_copy(it, chunk).start()

        @pl.when(me > 0)
        def _():
            down_copy(it, chunk).start()

    def smooth(it, chunk):
        rows = slice(chunk * tall, (chunk + 1) * tall)

        @pl.when(me > 0)
        def _():
            up_copy(it, chunk).wait_recv()

        @pl.when(me < count - 1)
        def _():
            down_copy(it, chunk).wait_recv()

        for part in range(2):
            fresh = (
                mixed(summed[it, chunk, part], 0)
                + mixed(from_low[it, chunk, part], -channels)
                + mixed(from_high[it, chunk, part], channels)
            )
            off = gain[it + 1, part, rows] - fresh
            moved = fresh - cons[part, rows]
            dual[part, rows] = dual[part, rows] + off
            cons[part, rows] = fresh
            sums[2 * it : 2 * it + 1] += jnp.sum(off * off, 0, keepdims=True)
            sums[2 * it + 1 : 2 * it + 2] += jnp.sum(moved * moved, 0, keepdims=True)

    def norm_copy(step):
        return pltpu.make_async_remote_copy(
            src_ref=sums, dst_ref=slots.at[me],
            send_sem=norm_send.at[step], recv_sem=norm_recv.at[step],
            device_id={"chan": lax.rem(me + step, count)}, device_id_type=MESH,
        )

    def put(target, state):
        for part in range(2):
            target[part] = jnp.transpose(state[part])[:, 0:width].reshape(pols, dirs, channels, width)

    steps = PITCH // GROUP // CHUNKS
    for it in range(ITERS):
        for chunk in range(CHUNKS):
            lax.fori_loop(chunk * steps, (chunk + 1) * steps, functools.partial(sweep, it), 0)
            if it == 0 and chunk == 0:
                pl.semaphore_wait(barrier, count - 1)
            if it > 0:
                smooth(it - 1, chunk)
            finish(it, chunk)
    put(jones_out, gain.at[ITERS])
    for chunk in range(CHUNKS):
        smooth(ITERS - 1, chunk)

    slots[pl.ds(me, 1)] = sums[...][None]
    for step in range(1, count):
        norm_copy(step).start()
    put(consensus_out, cons)
    put(duals_out, dual)

    for it in range(ITERS):
        for chunk in range(CHUNKS):

            @pl.when(me < count - 1)
            def _():
                up_copy(it, chunk).wait_send()

            @pl.when(me > 0)
            def _():
                down_copy(it, chunk).wait_send()

    for step in range(1, count):
        norm_copy(step).wait()
    gathered = slots[0]
    for j in range(1, count):
        gathered = gathered + slots[j]
    folded = jnp.sum(gathered, axis=1, keepdims=True) * (1.0 / entries)
    for it in range(ITERS):
        norms_out[it : it + 1, 0:1] = folded[2 * it : 2 * it + 1]
        norms_out[it : it + 1, 1:2] = folded[2 * it + 1 : 2 * it + 2] * (penalty * penalty)


def deliver(*refs):
    sources, targets, sem = refs[0:4], refs[4:8], refs[8]
    copies = [pltpu.make_async_copy(s, t, sem.at[i]) for i, (s, t) in enumerate(zip(sources, targets))]
    for copy in copies:
        copy.start()
    for copy in copies:
        copy.wait()


def solution(mesh):
    count = mesh.shape["chan"]

    def local(visibility, coherency, jones_start, duals_start):
        _, pols, dirs, channels, width = jones_start.shape
        pairs = visibility.shape[-1]
        times = visibility.shape[3]
        lanes = pols * dirs * channels
        assert times == 1 and pols == 2 and channels == 4 and lanes == 128 and width <= PITCH - 2 and width % 2 == 0
        tiles = pl.cdiv(pairs, 128)
        whole = pairs // 128
        entries = jones_start.size * count
        sky = coherency.transpose(0, 1, 2, 4, 3, 5).reshape(2, pols, dirs, channels, pairs)
        state = jax.ShapeDtypeStruct(jones_start.shape, jnp.float32)
        f32, bf16 = jnp.float32, jnp.bfloat16
        rows = PITCH // CHUNKS
        shapes = (state, state, state, jax.ShapeDtypeStruct((ITERS, 2), f32))
        packed = (2, PITCH, lanes)
        halo = (ITERS, CHUNKS, 2, rows, lanes)
        results = pl.pallas_call(
            functools.partial(kernel, count, (pols, dirs, channels, width, pairs, entries)),
            out_shape=shapes,
            in_specs=[pl.BlockSpec(memory_space=pl.ANY)] * 4,
            out_specs=tuple([pl.BlockSpec(memory_space=pltpu.VMEM)] * 4),
            scratch_shapes=[
                pltpu.VMEM(visibility.shape, f32),
                pltpu.VMEM((tiles, 2, pols, dirs, channels, 128), bf16),
                pltpu.VMEM((2, pols, dirs, channels, pairs - 128 * whole), bf16),
                pltpu.VMEM(jones_start.shape, f32),
                pltpu.VMEM(duals_start.shape, f32),
                pltpu.VMEM((2, 2 * channels, tiles * 128), f32),
                pltpu.VMEM((2 * PITCH, 256), jnp.int32),
                pltpu.VMEM((2 * lanes, lanes), bf16),
                pltpu.VMEM((2, PITCH, PITCH, lanes), f32),
                pltpu.VMEM((2, PITCH, PITCH, lanes), f32),
                pltpu.VMEM((2, GROUP, PITCH, lanes), f32),
                pltpu.VMEM((2, GROUP, PITCH, lanes), f32),
                pltpu.VMEM((3, PITCH, lanes), f32),
                pltpu.VMEM((ITERS + 1,) + packed, f32),
                pltpu.VMEM(packed, f32),
                pltpu.VMEM(packed, f32),
                pltpu.VMEM(halo, f32),
                pltpu.VMEM(halo, f32),
                pltpu.VMEM(halo, f32),
                pltpu.VMEM((8, lanes), f32),
                pltpu.VMEM((count, 8, lanes), f32),
                pltpu.SemaphoreType.DMA((3,)),
                pltpu.SemaphoreType.DMA((whole,)),
                pltpu.SemaphoreType.DMA,
                pltpu.SemaphoreType.DMA((ITERS, CHUNKS, 2)),
                pltpu.SemaphoreType.DMA((ITERS, CHUNKS)),
                pltpu.SemaphoreType.DMA((ITERS, CHUNKS)),
                pltpu.SemaphoreType.DMA((count,)),
                pltpu.SemaphoreType.DMA((count,)),
            ],
            compiler_params=pltpu.CompilerParams(
                collective_id=0, has_side_effects=True, vmem_limit_bytes=60 * 1024 * 1024
            ),
        )(visibility, sky, jones_start, duals_start)
        return pl.pallas_call(
            deliver,
            out_shape=shapes,
            in_specs=[pl.BlockSpec(memory_space=pl.ANY)] * 4,
            out_specs=tuple([pl.BlockSpec(memory_space=pl.ANY)] * 4),
            scratch_shapes=[pltpu.SemaphoreType.DMA((4,))],
        )(*results)

    placed = (
        P(None, None, "chan", "slot", None),
        P(None, None, None, "chan", "slot", None),
        P(None, None, "slot", "chan", None),
        P(None, None, "slot", "chan", None),
    )
    return jax.shard_map(
        local,
        mesh=mesh,
        in_specs=placed,
        out_specs=(
            P(None, None, "slot", "chan", None),
            P(None, None, "slot", "chan", None),
            P(None, None, "slot", "chan", None),
            P("slot", None),
        ),
        check_vma=False,
    )
```

```python
import functools

import jax
import jax.numpy as jnp
from jax import lax
from jax.experimental import pallas as pl
from jax.experimental.pallas import tpu as pltpu
from jax.sharding import PartitionSpec as P

ITERS = 2
PITCH = 64
GROUP = 8
CHUNKS = 2
MESH = pl.DeviceIdType.MESH

penalty = 8.0
kernel_taps = (0.04, 0.06, 0.1, 0.15, 0.3, 0.15, 0.1, 0.06, 0.04)


def kernel(
    count, dims,
    vis_in, sky_in, jones_in, duals_in,
    jones_out, consensus_out, duals_out, norms_out,
    vis_raw, sky_raw, tail_raw, jones_raw, duals_raw,
    vis_rows, base, mixer, sky, vis, z_keep, rest, acc,
    gain, cons, dual, summed, from_low, from_high, sums, slots,
    load_sem, sky_sem, tail_sem, send_sem, low_sem, high_sem, norm_send, norm_recv,
):
    pols, dirs, channels, width, pairs, entries = dims
    lanes = pols * dirs * channels
    tiles = pl.cdiv(pairs, 128)
    whole = pairs // 128
    me = lax.axis_index("chan")

    loads = [
        pltpu.make_async_copy(source, target, load_sem.at[i])
        for i, (source, target) in enumerate(((vis_in, vis_raw), (jones_in, jones_raw), (duals_in, duals_raw)))
    ]
    sky_loads = [
        pltpu.make_async_copy(sky_in.at[:, :, :, :, 128 * j : 128 * j + 128], sky_raw.at[j], sky_sem.at[j])
        for j in range(whole)
    ]
    tail_load = pltpu.make_async_copy(sky_in.at[:, :, :, :, 128 * whole : pairs], tail_raw, tail_sem)
    for copy in loads + sky_loads + [tail_load]:
        copy.start()

    from_low[...] = jnp.zeros_like(from_low)
    from_high[...] = jnp.zeros_like(from_high)
    barrier = pltpu.get_barrier_semaphore()
    for step in range(1, count):
        pl.semaphore_signal(barrier, inc=1, device_id={"chan": lax.rem(me + step, count)}, device_id_type=MESH)

    sums[...] = jnp.zeros_like(sums)
    sky_raw[whole] = jnp.zeros(sky_raw.shape[1:], sky_raw.dtype)
    sky[:, width:] = jnp.zeros((2, PITCH - width, PITCH, lanes), jnp.float32)
    vis[:, width:] = jnp.zeros((2, PITCH - width, PITCH, lanes), jnp.float32)
    vis_rows[:, :, 128 * whole :] = jnp.zeros((2, 2 * channels, 128 * (tiles - whole)), jnp.float32)
    row = lax.broadcasted_iota(jnp.int32, (2 * PITCH, 256), 0)
    col = lax.broadcasted_iota(jnp.int32, (2 * PITCH, 256), 1)
    station = row & (PITCH - 1)
    target = jnp.where(row >= PITCH, station + width, station)
    base[...] = jnp.where(station < width, col - target, -1024)
    row = lax.broadcasted_iota(jnp.int32, (2 * lanes, lanes), 0) & (lanes - 1)
    col = lax.broadcasted_iota(jnp.int32, (2 * lanes, lanes), 1)
    half = dirs * channels
    same = ((row >= half) == (col >= half)) & ((row & (channels - 1)) == (col & (channels - 1)))
    mixer[...] = jnp.where(same, -1.0, 0.0).astype(jnp.bfloat16)

    def chooser(i):
        return jnp.where(base[...] == (2 * width * i) % 128, 1.0, 0.0).astype(jnp.bfloat16)

    def swung(left, right):
        return lax.dot_general(left, right, (((1,), (1,)), ((), ())), preferred_element_type=jnp.float32)

    loads[0].wait()
    for part in range(2):
        for pol in range(pols):
            for f in range(channels):
                vis_rows[part, pol * channels + f : pol * channels + f + 1, 0:pairs] = vis_raw[part, pol, f]
    upper = lax.broadcasted_iota(jnp.int32, (2 * channels, 256), 0) < channels
    lane = lax.broadcasted_iota(jnp.int32, (2 * PITCH, lanes), 1)
    real = (lane & 8) == 0
    gap = jnp.zeros((half - 16, 256), jnp.float32)
    for i in range(width // 2):
        j = (2 * width * i) // 128
        first, second = [], []
        for part in range(2):
            value = vis_rows[part, :, 128 * j : 128 * j + 256]
            high = value.astype(jnp.bfloat16).astype(jnp.float32)
            low = pltpu.roll(value - high, channels, 0)
            first.append(jnp.where(upper, high, low))
            second.append(jnp.where(upper, low, high))
        right = jnp.concatenate(first + [gap] + second + [gap], 0).astype(jnp.bfloat16)
        turned = swung(chooser(i), right)
        vis[0, 2 * i : 2 * i + 2] = jnp.where(real, turned, 0.0).reshape(2, PITCH, lanes)
        vis[1, 2 * i : 2 * i + 2] = jnp.where(real, 0.0, turned).reshape(2, PITCH, lanes)

    for copy in loads[1:]:
        copy.wait()
    for part in range(2):
        start = jnp.transpose(jones_raw[part].reshape(lanes, width))
        gain[0, part, 0:width] = start
        cons[part, 0:width] = start
        dual[part, 0:width] = jnp.transpose(duals_raw[part].reshape(lanes, width))
        empty = jnp.zeros((PITCH - width, lanes), jnp.float32)
        gain[0, part, width:] = empty
        cons[part, width:] = empty
        dual[part, width:] = empty

    for j in range(whole):
        sky_loads[j].wait()
    tail_load.wait()
    sky_raw[whole, :, :, :, :, 0 : pairs - 128 * whole] = tail_raw[...]
    for i in range(width // 2):
        j = (2 * width * i) // 128
        right = jnp.concatenate(
            [sky_raw[j].reshape(2 * lanes, 128), sky_raw[j + 1].reshape(2 * lanes, 128)], 1
        )
        turned = swung(chooser(i), right)
        for part in range(2):
            sky[part, 2 * i : 2 * i + 2] = turned[:, part * lanes : (part + 1) * lanes].reshape(2, PITCH, lanes)
            for p in (2 * i, 2 * i + 1):
                sky[part, p, p : p + 1] = jnp.zeros((1, lanes), jnp.float32)

    def parted(value):
        high = value.astype(jnp.bfloat16)
        low = (value - high.astype(jnp.float32)).astype(jnp.bfloat16)
        return jnp.concatenate([high, low], 1)

    def sweep(it, block, carry):
        gr, gi = gain[it, 0], gain[it, 1]
        sides = ([], [])
        for b in range(GROUP):
            p = block * GROUP + b
            sr, si = sky[0, p], sky[1, p]
            zr = sr * gr + si * gi
            zi = sr * gi - si * gr
            z_keep[0, b] = zr
            z_keep[1, b] = zi
            lr, li = gain[it, 0, pl.ds(p, 1)], gain[it, 1, pl.ds(p, 1)]
            sides[0].append(parted(lr * zr + li * zi - vis[0, p]))
            sides[1].append(parted(li * zr - lr * zi - vis[1, p]))
        for part in range(2):
            rest[part] = jnp.dot(
                jnp.concatenate(sides[part], 0), mixer[...], preferred_element_type=jnp.float32
            ).reshape(GROUP, PITCH, lanes)
        sums_of = ([], [], [])
        for b in range(GROUP):
            zr, zi = z_keep[0, b], z_keep[1, b]
            dr, di = rest[0, b], rest[1, b]
            for i, value in enumerate((dr * zr - di * zi, dr * zi + di * zr, zr * zr + zi * zi)):
                sums_of[i].append(jnp.sum(value, 0, keepdims=True))
        for i in range(3):
            acc[i, pl.ds(pl.multiple_of(block * GROUP, GROUP), GROUP)] = jnp.concatenate(sums_of[i], 0)
        return carry

    tall = PITCH // CHUNKS
    place = lax.broadcasted_iota(jnp.int32, (tall, lanes), 1) & (channels - 1)

    def mixed(block, distance):
        out = None
        for shift in range(1 - channels, channels):
            offset = distance + shift + 4
            if offset < 0 or offset > 8:
                continue
            inside = (place + shift >= 0) & (place + shift < channels)
            weight = jnp.where(inside, kernel_taps[offset], 0.0)
            moved = block if shift == 0 else pltpu.roll(block, (-shift) % lanes, 1)
            term = weight * moved
            out = term if out is None else out + term
        return out

    def up_copy(it, chunk):
        return pltpu.make_async_remote_copy(
            src_ref=summed.at[it, chunk], dst_ref=from_low.at[it, chunk],
            send_sem=send_sem.at[it, chunk, 0], recv_sem=low_sem.at[it, chunk],
            device_id={"chan": lax.rem(me + 1, count)}, device_id_type=MESH,
        )

    def down_copy(it, chunk):
        return pltpu.make_async_remote_copy(
            src_ref=summed.at[it, chunk], dst_ref=from_high.at[it, chunk],
            send_sem=send_sem.at[it, chunk, 1], recv_sem=high_sem.at[it, chunk],
            device_id={"chan": lax.rem(me + count - 1, count)}, device_id_type=MESH,
        )

    def finish(it, chunk):
        rows = slice(chunk * tall, (chunk + 1) * tall)
        lower = acc[2, rows]
        scale = lower + penalty
        for part in range(2):
            goal = cons[part, rows] - dual[part, rows]
            fresh = (acc[part, rows] + gain[it, part, rows] * lower + penalty * goal) / scale
            gain[it + 1, part, rows] = fresh
            summed[it, chunk, part] = fresh + dual[part, rows]

        @pl.when(me < count - 1)
        def _():
            up_copy(it, chunk).start()

        @pl.when(me > 0)
        def _():
            down_copy(it, chunk).start()

    def smooth(it, chunk):
        rows = slice(chunk * tall, (chunk + 1) * tall)

        @pl.when(me > 0)
        def _():
            up_copy(it, chunk).wait_recv()

        @pl.when(me < count - 1)
        def _():
            down_copy(it, chunk).wait_recv()

        for part in range(2):
            fresh = (
                mixed(summed[it, chunk, part], 0)
                + mixed(from_low[it, chunk, part], -channels)
                + mixed(from_high[it, chunk, part], channels)
            )
            off = gain[it + 1, part, rows] - fresh
            moved = fresh - cons[part, rows]
            dual[part, rows] = dual[part, rows] + off
            cons[part, rows] = fresh
            sums[2 * it : 2 * it + 1] += jnp.sum(off * off, 0, keepdims=True)
            sums[2 * it + 1 : 2 * it + 2] += jnp.sum(moved * moved, 0, keepdims=True)

    def norm_copy(step):
        return pltpu.make_async_remote_copy(
            src_ref=sums, dst_ref=slots.at[me],
            send_sem=norm_send.at[step], recv_sem=norm_recv.at[step],
            device_id={"chan": lax.rem(me + step, count)}, device_id_type=MESH,
        )

    def put(target, state):
        for part in range(2):
            target[part] = jnp.transpose(state[part])[:, 0:width].reshape(pols, dirs, channels, width)

    steps = PITCH // GROUP // CHUNKS
    for it in range(ITERS):
        for chunk in range(CHUNKS):
            lax.fori_loop(chunk * steps, (chunk + 1) * steps, functools.partial(sweep, it), 0)
            if it == 0 and chunk == 0:
                pl.semaphore_wait(barrier, count - 1)
            if it > 0:
                smooth(it - 1, chunk)
            finish(it, chunk)
    put(jones_out, gain.at[ITERS])
    for chunk in range(CHUNKS):
        smooth(ITERS - 1, chunk)

    slots[pl.ds(me, 1)] = sums[...][None]
    for step in range(1, count):
        norm_copy(step).start()
    put(consensus_out, cons)
    put(duals_out, dual)

    for it in range(ITERS):
        for chunk in range(CHUNKS):

            @pl.when(me < count - 1)
            def _():
                up_copy(it, chunk).wait_send()

            @pl.when(me > 0)
            def _():
                down_copy(it, chunk).wait_send()

    for step in range(1, count):
        norm_copy(step).wait()
    gathered = slots[0]
    for j in range(1, count):
        gathered = gathered + slots[j]
    folded = jnp.sum(gathered, axis=1, keepdims=True) * (1.0 / entries)
    for it in range(ITERS):
        norms_out[it : it + 1, 0:1] = folded[2 * it : 2 * it + 1]
        norms_out[it : it + 1, 1:2] = folded[2 * it + 1 : 2 * it + 2] * (penalty * penalty)


def deliver(*refs):
    sources, targets, sem = refs[0:4], refs[4:8], refs[8]
    copies = [pltpu.make_async_copy(s, t, sem.at[i]) for i, (s, t) in enumerate(zip(sources, targets))]
    for copy in copies:
        copy.start()
    for copy in copies:
        copy.wait()


def solution(mesh):
    count = mesh.shape["chan"]

    def local(visibility, coherency, jones_start, duals_start):
        _, pols, dirs, channels, width = jones_start.shape
        pairs = visibility.shape[-1]
        times = visibility.shape[3]
        lanes = pols * dirs * channels
        assert times == 1 and pols == 2 and channels == 4 and lanes == 128 and width <= PITCH - 2 and width % 2 == 0
        tiles = pl.cdiv(pairs, 128)
        whole = pairs // 128
        entries = jones_start.size * count
        sky = coherency.transpose(0, 1, 2, 4, 3, 5).reshape(2, pols, dirs, channels, pairs)
        state = jax.ShapeDtypeStruct(jones_start.shape, jnp.float32)
        f32, bf16 = jnp.float32, jnp.bfloat16
        rows = PITCH // CHUNKS
        shapes = (state, state, state, jax.ShapeDtypeStruct((ITERS, 2), f32))
        packed = (2, PITCH, lanes)
        halo = (ITERS, CHUNKS, 2, rows, lanes)
        results = pl.pallas_call(
            functools.partial(kernel, count, (pols, dirs, channels, width, pairs, entries)),
            out_shape=shapes,
            in_specs=[pl.BlockSpec(memory_space=pl.ANY)] * 4,
            out_specs=tuple([pl.BlockSpec(memory_space=pltpu.VMEM)] * 4),
            scratch_shapes=[
                pltpu.VMEM(visibility.shape, f32),
                pltpu.VMEM((tiles, 2, pols, dirs, channels, 128), bf16),
                pltpu.VMEM((2, pols, dirs, channels, pairs - 128 * whole), bf16),
                pltpu.VMEM(jones_start.shape, f32),
                pltpu.VMEM(duals_start.shape, f32),
                pltpu.VMEM((2, 2 * channels, tiles * 128), f32),
                pltpu.VMEM((2 * PITCH, 256), jnp.int32),
                pltpu.VMEM((2 * lanes, lanes), bf16),
                pltpu.VMEM((2, PITCH, PITCH, lanes), f32),
                pltpu.VMEM((2, PITCH, PITCH, lanes), f32),
                pltpu.VMEM((2, GROUP, PITCH, lanes), f32),
                pltpu.VMEM((2, GROUP, PITCH, lanes), f32),
                pltpu.VMEM((3, PITCH, lanes), f32),
                pltpu.VMEM((ITERS + 1,) + packed, f32),
                pltpu.VMEM(packed, f32),
                pltpu.VMEM(packed, f32),
                pltpu.VMEM(halo, f32),
                pltpu.VMEM(halo, f32),
                pltpu.VMEM(halo, f32),
                pltpu.VMEM((8, lanes), f32),
                pltpu.VMEM((count, 8, lanes), f32),
                pltpu.SemaphoreType.DMA((3,)),
                pltpu.SemaphoreType.DMA((whole,)),
                pltpu.SemaphoreType.DMA,
                pltpu.SemaphoreType.DMA((ITERS, CHUNKS, 2)),
                pltpu.SemaphoreType.DMA((ITERS, CHUNKS)),
                pltpu.SemaphoreType.DMA((ITERS, CHUNKS)),
                pltpu.SemaphoreType.DMA((count,)),
                pltpu.SemaphoreType.DMA((count,)),
            ],
            compiler_params=pltpu.CompilerParams(
                collective_id=0, has_side_effects=True, vmem_limit_bytes=24 * 1024 * 1024
            ),
        )(*[pltpu.with_memory_space_constraint(x, pltpu.HBM) for x in (visibility, sky, jones_start, duals_start)])
        return pl.pallas_call(
            deliver,
            out_shape=shapes,
            in_specs=[pl.BlockSpec(memory_space=pltpu.VMEM)] * 4,
            out_specs=tuple([pl.BlockSpec(memory_space=pl.ANY)] * 4),
            scratch_shapes=[pltpu.SemaphoreType.DMA((4,))],
            compiler_params=pltpu.CompilerParams(vmem_limit_bytes=4 * 1024 * 1024),
        )(*results)

    placed = (
        P(None, None, "chan", "slot", None),
        P(None, None, None, "chan", "slot", None),
        P(None, None, "slot", "chan", None),
        P(None, None, "slot", "chan", None),
    )
    return jax.shard_map(
        local,
        mesh=mesh,
        in_specs=placed,
        out_specs=(
            P(None, None, "slot", "chan", None),
            P(None, None, "slot", "chan", None),
            P(None, None, "slot", "chan", None),
            P("slot", None),
        ),
        check_vma=False,
    )
```

```python
import functools

import jax
import jax.numpy as jnp
from jax import lax
from jax.experimental import pallas as pl
from jax.experimental.pallas import tpu as pltpu
from jax.sharding import PartitionSpec as P

ITERS = 2
PITCH = 64
GROUP = 8
CHUNKS = ((0, 32), (32, 56), (56, 64))
MESH = pl.DeviceIdType.MESH

penalty = 8.0
kernel_taps = (0.04, 0.06, 0.1, 0.15, 0.3, 0.15, 0.1, 0.06, 0.04)


def kernel(
    count, dims,
    vis_in, sky_in, jones_in, duals_in,
    jones_out, consensus_out, duals_out, norms_out,
    vis_raw, sky_raw, tail_raw, jones_raw, duals_raw,
    vis_rows, chooser, mixer, sky, vis, z_keep, rest, acc,
    gain, cons, dual, summed, from_low, from_high, sums, partial, slots,
    load_sem, sky_sem, tail_sem, send_sem, low_sem, high_sem, norm_send, norm_recv,
):
    pols, dirs, channels, width, pairs, entries = dims
    lanes = pols * dirs * channels
    tiles = pl.cdiv(pairs, 128)
    whole = pairs // 128
    me = lax.axis_index("chan")

    loads = [
        pltpu.make_async_copy(source, target, load_sem.at[i])
        for i, (source, target) in enumerate(((vis_in, vis_raw), (jones_in, jones_raw), (duals_in, duals_raw)))
    ]
    sky_loads = [
        pltpu.make_async_copy(sky_in.at[:, :, :, :, 128 * j : 128 * j + 128], sky_raw.at[j], sky_sem.at[j])
        for j in range(whole)
    ]
    tail_load = pltpu.make_async_copy(sky_in.at[:, :, :, :, 128 * whole : pairs], tail_raw, tail_sem)
    for copy in loads + sky_loads + [tail_load]:
        copy.start()

    from_low[...] = jnp.zeros_like(from_low)
    from_high[...] = jnp.zeros_like(from_high)
    barrier = pltpu.get_barrier_semaphore()
    for step in range(1, count):
        pl.semaphore_signal(barrier, inc=1, device_id={"chan": lax.rem(me + step, count)}, device_id_type=MESH)

    sums[...] = jnp.zeros_like(sums)
    sky_raw[whole] = jnp.zeros(sky_raw.shape[1:], sky_raw.dtype)
    sky[:, width:] = jnp.zeros((2, PITCH - width, PITCH, lanes), jnp.float32)
    vis[:, width:] = jnp.zeros((2, PITCH - width, PITCH, lanes), jnp.float32)
    vis_rows[:, :, 128 * whole :] = jnp.zeros((2, 2 * channels, 128 * (tiles - whole)), jnp.float32)
    row = lax.broadcasted_iota(jnp.int32, (2 * PITCH, 128), 0)
    col = lax.broadcasted_iota(jnp.int32, (2 * PITCH, 128), 1)
    station = row & (PITCH - 1)
    target = jnp.where(row >= PITCH, station + width, station)
    chooser[...] = jnp.where((station < width) & (col == target), 1.0, 0.0).astype(jnp.bfloat16)
    row = lax.broadcasted_iota(jnp.int32, (2 * lanes, lanes), 0) & (lanes - 1)
    col = lax.broadcasted_iota(jnp.int32, (2 * lanes, lanes), 1)
    half = dirs * channels
    same = ((row >= half) == (col >= half)) & ((row & (channels - 1)) == (col & (channels - 1)))
    mixer[...] = jnp.where(same, -1.0, 0.0).astype(jnp.bfloat16)

    def window(first, second, i, start=None):
        offset = (2 * width * i) % 128
        if offset == 0:
            return first
        back = 128 - offset
        lane = lax.broadcasted_iota(jnp.int32, first.shape, 1)
        return jnp.where(lane < back, pltpu.roll(first, back, 1), pltpu.roll(second, back, 1))

    def swung(right):
        return lax.dot_general(chooser[...], right, (((1,), (1,)), ((), ())), preferred_element_type=jnp.float32)

    loads[0].wait()
    for part in range(2):
        for pol in range(pols):
            for f in range(channels):
                vis_rows[part, pol * channels + f : pol * channels + f + 1, 0:pairs] = vis_raw[part, pol, f]
    upper = lax.broadcasted_iota(jnp.int32, (2 * channels, 128), 0) < channels
    lane = lax.broadcasted_iota(jnp.int32, (2 * PITCH, lanes), 1)
    real = (lane & 8) == 0
    gap = jnp.zeros((half - 16, 128), jnp.float32)

    def vis_side(i):
        j = (2 * width * i) // 128
        first, second = [], []
        for part in range(2):
            value = window(vis_rows[part, :, 128 * j : 128 * j + 128], vis_rows[part, :, 128 * j + 128 : 128 * j + 256], i)
            high = value.astype(jnp.bfloat16).astype(jnp.float32)
            low = pltpu.roll(value - high, channels, 0)
            first.append(jnp.where(upper, high, low))
            second.append(jnp.where(upper, low, high))
        return jnp.concatenate(first + [gap] + second + [gap], 0).astype(jnp.bfloat16)

    for i in range(0, width // 2, 2):
        both = range(i, min(i + 2, width // 2))
        turned = swung(jnp.concatenate([vis_side(k) for k in both], 0))
        for n, k in enumerate(both):
            mine = turned[:, n * lanes : (n + 1) * lanes]
            vis[0, 2 * k : 2 * k + 2] = jnp.where(real, mine, 0.0).reshape(2, PITCH, lanes)
            vis[1, 2 * k : 2 * k + 2] = jnp.where(real, 0.0, mine).reshape(2, PITCH, lanes)

    for copy in loads[1:]:
        copy.wait()
    for part in range(2):
        start = jnp.transpose(jones_raw[part].reshape(lanes, width))
        gain[0, part, 0:width] = start
        cons[part, 0:width] = start
        dual[part, 0:width] = jnp.transpose(duals_raw[part].reshape(lanes, width))
        empty = jnp.zeros((PITCH - width, lanes), jnp.float32)
        gain[0, part, width:] = empty
        cons[part, width:] = empty
        dual[part, width:] = empty

    done = [0]

    def turn(block):
        pairs_to = range(block * GROUP // 2, min((block + 1) * GROUP // 2, width // 2))
        last = min((2 * width * pairs_to[-1]) // 128 + 1, whole)
        while done[0] <= last:
            if done[0] < whole:
                sky_loads[done[0]].wait()
            else:
                tail_load.wait()
                sky_raw[whole, :, :, :, :, 0 : pairs - 128 * whole] = tail_raw[...]
            done[0] += 1
        for i in pairs_to:
            j = (2 * width * i) // 128
            turned = swung(window(sky_raw[j].reshape(2 * lanes, 128), sky_raw[j + 1].reshape(2 * lanes, 128), i))
            for part in range(2):
                sky[part, 2 * i : 2 * i + 2] = turned[:, part * lanes : (part + 1) * lanes].reshape(2, PITCH, lanes)
                for p in (2 * i, 2 * i + 1):
                    sky[part, p, p : p + 1] = jnp.zeros((1, lanes), jnp.float32)

    def parted(value):
        high = value.astype(jnp.bfloat16)
        low = (value - high.astype(jnp.float32)).astype(jnp.bfloat16)
        return jnp.concatenate([high, low], 1)

    def gathered_rows(values):
        row = lax.broadcasted_iota(jnp.int32, (8, lanes), 0)
        for bit in (1, 2, 4):
            even = (row & bit) == 0
            values = [
                jnp.where(even, a, b) + pltpu.roll(jnp.where(even, b, a), bit, 0)
                for a, b in zip(values[0::2], values[1::2])
            ]
        return values[0]

    def sweep(it, block, carry):
        gr, gi = gain[it, 0], gain[it, 1]
        sides = ([], [])
        for b in range(GROUP):
            p = block * GROUP + b
            sr, si = sky[0, p], sky[1, p]
            zr = sr * gr + si * gi
            zi = sr * gi - si * gr
            z_keep[0, b] = zr
            z_keep[1, b] = zi
            lr, li = gain[it, 0, pl.ds(p, 1)], gain[it, 1, pl.ds(p, 1)]
            sides[0].append(parted(lr * zr + li * zi - vis[0, p]))
            sides[1].append(parted(li * zr - lr * zi - vis[1, p]))
        for part in range(2):
            rest[part] = jnp.dot(
                jnp.concatenate(sides[part], 0), mixer[...], preferred_element_type=jnp.float32
            ).reshape(GROUP, PITCH, lanes)
        sums_of = ([], [], [])
        for b in range(GROUP):
            zr, zi = z_keep[0, b], z_keep[1, b]
            dr, di = rest[0, b], rest[1, b]
            for i, value in enumerate((dr * zr - di * zi, dr * zi + di * zr, zr * zr + zi * zi)):
                sums_of[i].append(jnp.sum(value.reshape(PITCH // 8, 8, lanes), 0))
        for i in range(3):
            acc[i, pl.ds(pl.multiple_of(block * GROUP, GROUP), GROUP)] = gathered_rows(sums_of[i])
        return carry

    place = lax.broadcasted_iota(jnp.int32, (8, lanes), 1) & (channels - 1)

    def mixed(block, distance):
        out = None
        for shift in range(1 - channels, channels):
            offset = distance + shift + 4
            if offset < 0 or offset > 8:
                continue
            inside = (place + shift >= 0) & (place + shift < channels)
            weight = jnp.where(inside, kernel_taps[offset], 0.0)[0:1]
            moved = block if shift == 0 else pltpu.roll(block, (-shift) % lanes, 1)
            term = weight * moved
            out = term if out is None else out + term
        return out

    def up_copy(it, chunk):
        return pltpu.make_async_remote_copy(
            src_ref=summed.at[it, :, slice(*CHUNKS[chunk])], dst_ref=from_low.at[it, :, slice(*CHUNKS[chunk])],
            send_sem=send_sem.at[it, chunk, 0], recv_sem=low_sem.at[it, chunk],
            device_id={"chan": lax.rem(me + 1, count)}, device_id_type=MESH,
        )

    def down_copy(it, chunk):
        return pltpu.make_async_remote_copy(
            src_ref=summed.at[it, :, slice(*CHUNKS[chunk])], dst_ref=from_high.at[it, :, slice(*CHUNKS[chunk])],
            send_sem=send_sem.at[it, chunk, 1], recv_sem=high_sem.at[it, chunk],
            device_id={"chan": lax.rem(me + count - 1, count)}, device_id_type=MESH,
        )

    def finish(it, chunk):
        rows = slice(*CHUNKS[chunk])
        lower = acc[2, rows]
        scale = lower + penalty
        for part in range(2):
            goal = cons[part, rows] - dual[part, rows]
            fresh = (acc[part, rows] + gain[it, part, rows] * lower + penalty * goal) / scale
            gain[it + 1, part, rows] = fresh
            summed[it, part, rows] = fresh + dual[part, rows]

        @pl.when(me < count - 1)
        def _():
            up_copy(it, chunk).start()

        @pl.when(me > 0)
        def _():
            down_copy(it, chunk).start()

    def smooth(it, chunk):
        rows = slice(*CHUNKS[chunk])

        @pl.when(me > 0)
        def _():
            up_copy(it, chunk).wait_recv()

        @pl.when(me < count - 1)
        def _():
            down_copy(it, chunk).wait_recv()

        for part in range(2):
            fresh = (
                mixed(summed[it, part, rows], 0)
                + mixed(from_low[it, part, rows], -channels)
                + mixed(from_high[it, part, rows], channels)
            )
            off = gain[it + 1, part, rows] - fresh
            moved = fresh - cons[part, rows]
            dual[part, rows] = dual[part, rows] + off
            cons[part, rows] = fresh
            sums[2 * it] += jnp.sum((off * off).reshape(-1, 8, lanes), 0)
            sums[2 * it + 1] += jnp.sum((moved * moved).reshape(-1, 8, lanes), 0)

    def norm_copy(step):
        return pltpu.make_async_remote_copy(
            src_ref=partial, dst_ref=slots.at[me],
            send_sem=norm_send.at[step], recv_sem=norm_recv.at[step],
            device_id={"chan": lax.rem(me + step, count)}, device_id_type=MESH,
        )

    def put(target, state):
        for part in range(2):
            target[part] = jnp.transpose(state[part])[:, 0:width].reshape(pols, dirs, channels, width)

    turn(0)
    for it in range(ITERS):
        for chunk, (start, stop) in enumerate(CHUNKS):
            if it == 0:
                for block in range(start // GROUP, stop // GROUP):
                    if (block + 1) * GROUP < PITCH:
                        turn(block + 1)
                    sweep(it, block, 0)
            else:
                lax.fori_loop(start // GROUP, stop // GROUP, functools.partial(sweep, it), 0)
                smooth(it - 1, chunk)
            if it == 0 and chunk == 0:
                pl.semaphore_wait(barrier, count - 1)
            finish(it, chunk)
    put(jones_out, gain.at[ITERS])
    for chunk in range(len(CHUNKS)):
        smooth(ITERS - 1, chunk)

    lane = lax.broadcasted_iota(jnp.int32, (1, lanes), 1)
    share = lanes // (2 * ITERS)
    packed = jnp.zeros((1, lanes), jnp.float32)
    for i in range(2 * ITERS):
        value = jnp.sum(sums[i], 0, keepdims=True)
        stride = lanes // 2
        while stride >= share:
            value = value + pltpu.roll(value, stride, 1)
            stride //= 2
        packed = jnp.where(lane // share == i, value, packed)
    partial[...] = packed
    slots[pl.ds(me, 1)] = packed[None]
    for step in range(1, count):
        norm_copy(step).start()
    put(consensus_out, cons)
    put(duals_out, dual)

    for it in range(ITERS):
        for chunk in range(len(CHUNKS)):

            @pl.when(me < count - 1)
            def _():
                up_copy(it, chunk).wait_send()

            @pl.when(me > 0)
            def _():
                down_copy(it, chunk).wait_send()

    for step in range(1, count):
        norm_copy(step).wait()
    gathered = slots[0]
    for j in range(1, count):
        gathered = gathered + slots[j]
    for it in range(ITERS):
        for n, factor in enumerate((1.0, penalty * penalty)):
            mine = jnp.where(lane // share == 2 * it + n, gathered, 0.0)
            norms_out[it : it + 1, n : n + 1] = jnp.sum(mine, axis=1, keepdims=True) * (factor / entries)


def deliver(*refs):
    sources, targets, sem = refs[0:4], refs[4:8], refs[8]
    copies = [pltpu.make_async_copy(s, t, sem.at[i]) for i, (s, t) in enumerate(zip(sources, targets))]
    for copy in copies:
        copy.start()
    for copy in copies:
        copy.wait()


def solution(mesh):
    count = mesh.shape["chan"]

    def local(visibility, coherency, jones_start, duals_start):
        _, pols, dirs, channels, width = jones_start.shape
        pairs = visibility.shape[-1]
        times = visibility.shape[3]
        lanes = pols * dirs * channels
        assert times == 1 and pols == 2 and channels == 4 and lanes == 128 and width <= PITCH - 2 and width % 2 == 0
        tiles = pl.cdiv(pairs, 128)
        whole = pairs // 128
        entries = jones_start.size * count
        sky = coherency.transpose(0, 1, 2, 4, 3, 5).reshape(2, pols, dirs, channels, pairs)
        state = jax.ShapeDtypeStruct(jones_start.shape, jnp.float32)
        f32, bf16 = jnp.float32, jnp.bfloat16
        shapes = (state, state, state, jax.ShapeDtypeStruct((ITERS, 2), f32))
        packed = (2, PITCH, lanes)
        halo = (ITERS, 2, PITCH, lanes)
        parts = len(CHUNKS)
        results = pl.pallas_call(
            functools.partial(kernel, count, (pols, dirs, channels, width, pairs, entries)),
            out_shape=shapes,
            in_specs=[pl.BlockSpec(memory_space=pl.ANY)] * 4,
            out_specs=tuple([pl.BlockSpec(memory_space=pltpu.VMEM)] * 4),
            scratch_shapes=[
                pltpu.VMEM(visibility.shape, f32),
                pltpu.VMEM((tiles, 2, pols, dirs, channels, 128), bf16),
                pltpu.VMEM((2, pols, dirs, channels, pairs - 128 * whole), bf16),
                pltpu.VMEM(jones_start.shape, f32),
                pltpu.VMEM(duals_start.shape, f32),
                pltpu.VMEM((2, 2 * channels, tiles * 128), f32),
                pltpu.VMEM((2 * PITCH, 128), bf16),
                pltpu.VMEM((2 * lanes, lanes), bf16),
                pltpu.VMEM((2, PITCH, PITCH, lanes), f32),
                pltpu.VMEM((2, PITCH, PITCH, lanes), f32),
                pltpu.VMEM((2, GROUP, PITCH, lanes), f32),
                pltpu.VMEM((2, GROUP, PITCH, lanes), f32),
                pltpu.VMEM((3, PITCH, lanes), f32),
                pltpu.VMEM((ITERS + 1,) + packed, f32),
                pltpu.VMEM(packed, f32),
                pltpu.VMEM(packed, f32),
                pltpu.VMEM(halo, f32),
                pltpu.VMEM(halo, f32),
                pltpu.VMEM(halo, f32),
                pltpu.VMEM((2 * ITERS, 8, lanes), f32),
                pltpu.VMEM((1, lanes), f32),
                pltpu.VMEM((count, 1, lanes), f32),
                pltpu.SemaphoreType.DMA((3,)),
                pltpu.SemaphoreType.DMA((whole,)),
                pltpu.SemaphoreType.DMA,
                pltpu.SemaphoreType.DMA((ITERS, parts, 2)),
                pltpu.SemaphoreType.DMA((ITERS, parts)),
                pltpu.SemaphoreType.DMA((ITERS, parts)),
                pltpu.SemaphoreType.DMA((count,)),
                pltpu.SemaphoreType.DMA((count,)),
            ],
            compiler_params=pltpu.CompilerParams(
                collective_id=0, has_side_effects=True, vmem_limit_bytes=24 * 1024 * 1024
            ),
        )(*[pltpu.with_memory_space_constraint(x, pltpu.HBM) for x in (visibility, sky, jones_start, duals_start)])
        return pl.pallas_call(
            deliver,
            out_shape=shapes,
            in_specs=[pl.BlockSpec(memory_space=pltpu.VMEM)] * 4,
            out_specs=tuple([pl.BlockSpec(memory_space=pl.ANY)] * 4),
            scratch_shapes=[pltpu.SemaphoreType.DMA((4,))],
            compiler_params=pltpu.CompilerParams(vmem_limit_bytes=4 * 1024 * 1024),
        )(*results)

    placed = (
        P(None, None, "chan", "slot", None),
        P(None, None, None, "chan", "slot", None),
        P(None, None, "slot", "chan", None),
        P(None, None, "slot", "chan", None),
    )
    return jax.shard_map(
        local,
        mesh=mesh,
        in_specs=placed,
        out_specs=(
            P(None, None, "slot", "chan", None),
            P(None, None, "slot", "chan", None),
            P(None, None, "slot", "chan", None),
            P("slot", None),
        ),
        check_vma=False,
    )
```

```python
import functools

import jax
import jax.numpy as jnp
from jax import lax
from jax.experimental import pallas as pl
from jax.experimental.pallas import tpu as pltpu
from jax.sharding import PartitionSpec as P

ITERS = 2
PITCH = 64
GROUP = 8
TALL = 144
CHUNKS = ((0, 32), (32, 56), (56, 64))
MESH = pl.DeviceIdType.MESH

penalty = 8.0
kernel_taps = (0.04, 0.06, 0.1, 0.15, 0.3, 0.15, 0.1, 0.06, 0.04)


def kernel(
    count, dims,
    vis_in, sky_in, jones_in, duals_in,
    jones_out, consensus_out, duals_out, norms_out,
    vis_raw, sky_raw, tail_raw, jones_raw, duals_raw,
    vis_rows, chooser, placer, mixer, sky, vis, z_keep, rest, acc,
    gain, cons, dual, summed, from_low, from_high, sums, partial, slots,
    load_sem, sky_sem, tail_sem, send_sem, low_sem, high_sem, norm_send, norm_recv,
):
    pols, dirs, channels, width, pairs, entries = dims
    lanes = pols * dirs * channels
    tiles = pl.cdiv(pairs, 128)
    whole = pairs // 128
    me = lax.axis_index("chan")

    loads = [
        pltpu.make_async_copy(source, target, load_sem.at[i])
        for i, (source, target) in enumerate(((vis_in, vis_raw), (jones_in, jones_raw), (duals_in, duals_raw)))
    ]
    sky_loads = [
        pltpu.make_async_copy(sky_in.at[:, :, :, :, 128 * j : 128 * j + 128], sky_raw.at[j], sky_sem.at[j])
        for j in range(whole)
    ]
    tail_load = pltpu.make_async_copy(sky_in.at[:, :, :, :, 128 * whole : pairs], tail_raw, tail_sem)
    for copy in loads:
        copy.start()

    def issue(j, carry):
        start = pl.multiple_of(j * 128, 128)
        pltpu.make_async_copy(sky_in.at[:, :, :, :, pl.ds(start, 128)], sky_raw.at[j], sky_sem.at[j]).start()
        return carry

    lax.fori_loop(0, whole, issue, 0)
    tail_load.start()

    from_low[...] = jnp.zeros_like(from_low)
    from_high[...] = jnp.zeros_like(from_high)
    barrier = pltpu.get_barrier_semaphore()
    for step in range(1, count):
        pl.semaphore_signal(barrier, inc=1, device_id={"chan": lax.rem(me + step, count)}, device_id_type=MESH)
    sums[...] = jnp.zeros_like(sums)
    sky_raw[whole] = jnp.zeros(sky_raw.shape[1:], sky_raw.dtype)
    sky[:, width:] = jnp.zeros((2, PITCH - width, PITCH, lanes), jnp.float32)
    vis[:, width:] = jnp.zeros((2, PITCH - width, PITCH, lanes), jnp.float32)
    vis_rows[:, :, 128 * whole :] = jnp.zeros((2, 2 * channels, 128 * (tiles - whole)), jnp.float32)
    row = lax.broadcasted_iota(jnp.int32, (2 * PITCH, 128), 0)
    col = lax.broadcasted_iota(jnp.int32, (2 * PITCH, 128), 1)
    station = row & (PITCH - 1)
    target = jnp.where(row >= PITCH, station + width, station)
    chooser[...] = jnp.where((station < width) & (col == target), 1.0, 0.0).astype(jnp.bfloat16)
    def spot(pair):
        return pair + (PITCH - width) * (pair // width)

    bases = [spot(128 * j) // 8 * 8 for j in range(tiles)] + [width * PITCH]
    row = lax.broadcasted_iota(jnp.int32, (TALL, 128), 0).astype(jnp.float32)
    for j in range(tiles):
        pair = lax.broadcasted_iota(jnp.int32, (8, 128), 1).astype(jnp.float32) + 128.0 * j
        first = jnp.floor((pair + 0.5) * (1.0 / width))
        second = pair - first * width
        goal = pair + (PITCH - width) * first - bases[j]
        goal = jnp.where((first != second) & (first < width), goal, -1.0)
        placer[j] = jnp.where(row == goal[0:1], 1.0, 0.0).astype(jnp.bfloat16)
    row = lax.broadcasted_iota(jnp.int32, (2 * lanes, lanes), 0) & (lanes - 1)
    col = lax.broadcasted_iota(jnp.int32, (2 * lanes, lanes), 1)
    half = dirs * channels
    same = ((row >= half) == (col >= half)) & ((row & (channels - 1)) == (col & (channels - 1)))
    mixer[...] = jnp.where(same, -1.0, 0.0).astype(jnp.bfloat16)

    def window(first, second, i):
        offset = (2 * width * i) % 128
        if offset == 0:
            return first
        back = 128 - offset
        lane = lax.broadcasted_iota(jnp.int32, first.shape, 1)
        return jnp.where(lane < back, pltpu.roll(first, back, 1), pltpu.roll(second, back, 1))

    def swung(left, right):
        return lax.dot_general(left, right, (((1,), (1,)), ((), ())), preferred_element_type=jnp.float32)

    loads[0].wait()
    for part in range(2):
        for pol in range(pols):
            for f in range(channels):
                vis_rows[part, pol * channels + f : pol * channels + f + 1, 0:pairs] = vis_raw[part, pol, f]
    upper = lax.broadcasted_iota(jnp.int32, (2 * channels, 128), 0) < channels
    lane = lax.broadcasted_iota(jnp.int32, (2 * PITCH, lanes), 1)
    real = (lane & 8) == 0
    gap = jnp.zeros((half - 16, 128), jnp.float32)

    def vis_side(i):
        j = (2 * width * i) // 128
        first, second = [], []
        for part in range(2):
            value = window(vis_rows[part, :, 128 * j : 128 * j + 128], vis_rows[part, :, 128 * j + 128 : 128 * j + 256], i)
            high = value.astype(jnp.bfloat16).astype(jnp.float32)
            low = pltpu.roll(value - high, channels, 0)
            first.append(jnp.where(upper, high, low))
            second.append(jnp.where(upper, low, high))
        return jnp.concatenate(first + [gap] + second + [gap], 0).astype(jnp.bfloat16)

    for i in range(0, width // 2, 2):
        both = range(i, min(i + 2, width // 2))
        turned = swung(chooser[...], jnp.concatenate([vis_side(k) for k in both], 0))
        for n, k in enumerate(both):
            mine = turned[:, n * lanes : (n + 1) * lanes]
            vis[0, 2 * k : 2 * k + 2] = jnp.where(real, mine, 0.0).reshape(2, PITCH, lanes)
            vis[1, 2 * k : 2 * k + 2] = jnp.where(real, 0.0, mine).reshape(2, PITCH, lanes)

    for copy in loads[1:]:
        copy.wait()
    for part in range(2):
        start = jnp.transpose(jones_raw[part].reshape(lanes, width))
        gain[0, part, 0:width] = start
        cons[part, 0:width] = start
        dual[part, 0:width] = jnp.transpose(duals_raw[part].reshape(lanes, width))
        empty = jnp.zeros((PITCH - width, lanes), jnp.float32)
        gain[0, part, width:] = empty
        cons[part, width:] = empty
        dual[part, width:] = empty

    for copy in sky_loads + [tail_load]:
        copy.wait()
    sky_raw[whole, :, :, :, :, 0 : pairs - 128 * whole] = tail_raw[...]
    flat = sky.reshape(2, PITCH * PITCH, lanes)
    sky_flat = sky_raw.reshape(tiles, 2 * lanes, 128)
    state = {"tile": 0, "left": None}

    def turn(limit):
        while state["tile"] < tiles and bases[state["tile"]] < limit:
            j = state["tile"]
            turned = swung(placer[j], sky_flat[j])
            size = bases[j + 1] - bases[j]
            left = []
            for part in range(2):
                mine = turned[:, part * lanes : (part + 1) * lanes]
                head = mine[0:8]
                if state["left"] is not None:
                    head = head + state["left"][part]
                flat[part, bases[j] : bases[j] + 8] = head
                if size > 8:
                    flat[part, bases[j] + 8 : bases[j + 1]] = mine[8:size]
                left.append(mine[size : size + 8] if size + 8 <= TALL else None)
            state["tile"], state["left"] = j + 1, left

    def parted(value):
        high = value.astype(jnp.bfloat16)
        low = (value - high.astype(jnp.float32)).astype(jnp.bfloat16)
        return jnp.concatenate([high, low], 1)

    def gathered_rows(values):
        row = lax.broadcasted_iota(jnp.int32, (8, lanes), 0)
        for bit in (1, 2, 4):
            even = (row & bit) == 0
            values = [
                jnp.where(even, a, b) + pltpu.roll(jnp.where(even, b, a), bit, 0)
                for a, b in zip(values[0::2], values[1::2])
            ]
        return values[0]

    def front(it, block):
        gr, gi = gain[it, 0], gain[it, 1]
        bank = block % 2
        sides = ([], [])
        here = min(GROUP, width - block * GROUP)
        for b in range(here):
            p = block * GROUP + b
            sr, si = sky[0, p], sky[1, p]
            zr = sr * gr + si * gi
            zi = sr * gi - si * gr
            z_keep[bank, 0, b] = zr
            z_keep[bank, 1, b] = zi
            lr, li = gain[it, 0, p : p + 1], gain[it, 1, p : p + 1]
            sides[0].append(parted(lr * zr + li * zi - vis[0, p]))
            sides[1].append(parted(li * zr - lr * zi - vis[1, p]))
        for part in range(2):
            rest[bank, part, 0:here] = jnp.dot(
                jnp.concatenate(sides[part], 0), mixer[...], preferred_element_type=jnp.float32
            ).reshape(here, PITCH, lanes)

    def back(block):
        bank = block % 2
        sums_of = [[], [], []]
        for b in range(min(GROUP, width - block * GROUP)):
            zr, zi = z_keep[bank, 0, b], z_keep[bank, 1, b]
            dr, di = rest[bank, 0, b], rest[bank, 1, b]
            for i, value in enumerate((dr * zr - di * zi, dr * zi + di * zr, zr * zr + zi * zi)):
                sums_of[i].append(jnp.sum(value.reshape(PITCH // 8, 8, lanes), 0))
        for i in range(3):
            sums_of[i] += [jnp.zeros((8, lanes), jnp.float32)] * (GROUP - len(sums_of[i]))
            acc[i, block * GROUP : (block + 1) * GROUP] = gathered_rows(sums_of[i])

    place = lax.broadcasted_iota(jnp.int32, (8, lanes), 1) & (channels - 1)

    def mixed(block, distance):
        out = None
        for shift in range(1 - channels, channels):
            offset = distance + shift + 4
            if offset < 0 or offset > 8:
                continue
            inside = (place + shift >= 0) & (place + shift < channels)
            weight = jnp.where(inside, kernel_taps[offset], 0.0)[0:1]
            moved = block if shift == 0 else pltpu.roll(block, (-shift) % lanes, 1)
            term = weight * moved
            out = term if out is None else out + term
        return out

    def up_copy(it, chunk):
        return pltpu.make_async_remote_copy(
            src_ref=summed.at[it, :, slice(*CHUNKS[chunk])], dst_ref=from_low.at[it, :, slice(*CHUNKS[chunk])],
            send_sem=send_sem.at[it, chunk, 0], recv_sem=low_sem.at[it, chunk],
            device_id={"chan": lax.rem(me + 1, count)}, device_id_type=MESH,
        )

    def down_copy(it, chunk):
        return pltpu.make_async_remote_copy(
            src_ref=summed.at[it, :, slice(*CHUNKS[chunk])], dst_ref=from_high.at[it, :, slice(*CHUNKS[chunk])],
            send_sem=send_sem.at[it, chunk, 1], recv_sem=high_sem.at[it, chunk],
            device_id={"chan": lax.rem(me + count - 1, count)}, device_id_type=MESH,
        )

    def finish(it, chunk):
        rows = slice(*CHUNKS[chunk])
        lower = acc[2, rows]
        scale = lower + penalty
        for part in range(2):
            goal = cons[part, rows] - dual[part, rows]
            fresh = (acc[part, rows] + gain[it, part, rows] * lower + penalty * goal) / scale
            gain[it + 1, part, rows] = fresh
            summed[it, part, rows] = fresh + dual[part, rows]

        @pl.when(me < count - 1)
        def _():
            up_copy(it, chunk).start()

        @pl.when(me > 0)
        def _():
            down_copy(it, chunk).start()

    def smooth(it, chunk):
        rows = slice(*CHUNKS[chunk])

        @pl.when(me > 0)
        def _():
            up_copy(it, chunk).wait_recv()

        @pl.when(me < count - 1)
        def _():
            down_copy(it, chunk).wait_recv()

        for part in range(2):
            fresh = (
                mixed(summed[it, part, rows], 0)
                + mixed(from_low[it, part, rows], -channels)
                + mixed(from_high[it, part, rows], channels)
            )
            off = gain[it + 1, part, rows] - fresh
            moved = fresh - cons[part, rows]
            dual[part, rows] = dual[part, rows] + off
            cons[part, rows] = fresh
            sums[2 * it] += jnp.sum((off * off).reshape(-1, 8, lanes), 0)
            sums[2 * it + 1] += jnp.sum((moved * moved).reshape(-1, 8, lanes), 0)

    def norm_copy(step):
        return pltpu.make_async_remote_copy(
            src_ref=partial, dst_ref=slots.at[me],
            send_sem=norm_send.at[step], recv_sem=norm_recv.at[step],
            device_id={"chan": lax.rem(me + step, count)}, device_id_type=MESH,
        )

    def put(target, state):
        for part in range(2):
            target[part] = jnp.transpose(state[part])[:, 0:width].reshape(pols, dirs, channels, width)

    blocks = PITCH // GROUP
    stops = {stop // GROUP - 1: chunk for chunk, (_, stop) in enumerate(CHUNKS)}
    turn(GROUP * PITCH)
    for it in range(ITERS):
        front(it, 0)
        for block in range(blocks):
            if it == 0:
                turn((block + 2) * GROUP * PITCH)
            if block + 1 < blocks:
                front(it, block + 1)
            back(block)
            if block in stops:
                chunk = stops[block]
                if it > 0:
                    smooth(it - 1, chunk)
                if it == 0 and chunk == 0:
                    pl.semaphore_wait(barrier, count - 1)
                finish(it, chunk)
    put(jones_out, gain.at[ITERS])
    for chunk in range(len(CHUNKS)):
        smooth(ITERS - 1, chunk)

    lane = lax.broadcasted_iota(jnp.int32, (1, lanes), 1)
    share = lanes // (2 * ITERS)
    packed = jnp.zeros((1, lanes), jnp.float32)
    for i in range(2 * ITERS):
        value = jnp.sum(sums[i], 0, keepdims=True)
        stride = lanes // 2
        while stride >= share:
            value = value + pltpu.roll(value, stride, 1)
            stride //= 2
        packed = jnp.where(lane // share == i, value, packed)
    partial[...] = packed
    slots[pl.ds(me, 1)] = packed[None]
    for step in range(1, count):
        norm_copy(step).start()
    put(consensus_out, cons)
    put(duals_out, dual)

    for it in range(ITERS):
        for chunk in range(len(CHUNKS)):

            @pl.when(me < count - 1)
            def _():
                up_copy(it, chunk).wait_send()

            @pl.when(me > 0)
            def _():
                down_copy(it, chunk).wait_send()

    for step in range(1, count):
        norm_copy(step).wait()
    gathered = slots[0]
    for j in range(1, count):
        gathered = gathered + slots[j]
    for it in range(ITERS):
        for n, factor in enumerate((1.0, penalty * penalty)):
            mine = jnp.where(lane // share == 2 * it + n, gathered, 0.0)
            norms_out[it : it + 1, n : n + 1] = jnp.sum(mine, axis=1, keepdims=True) * (factor / entries)


def deliver(*refs):
    sources, targets, sem = refs[0:4], refs[4:8], refs[8]
    copies = [pltpu.make_async_copy(s, t, sem.at[i]) for i, (s, t) in enumerate(zip(sources, targets))]
    for copy in copies:
        copy.start()
    for copy in copies:
        copy.wait()


def solution(mesh):
    count = mesh.shape["chan"]

    def local(visibility, coherency, jones_start, duals_start):
        _, pols, dirs, channels, width = jones_start.shape
        pairs = visibility.shape[-1]
        times = visibility.shape[3]
        lanes = pols * dirs * channels
        assert times == 1 and pols == 2 and channels == 4 and lanes == 128 and width <= PITCH - 2 and width % 2 == 0
        tiles = pl.cdiv(pairs, 128)
        whole = pairs // 128
        entries = jones_start.size * count
        sky = coherency.transpose(0, 1, 2, 4, 3, 5).reshape(2, pols, dirs, channels, pairs)
        state = jax.ShapeDtypeStruct(jones_start.shape, jnp.float32)
        f32, bf16 = jnp.float32, jnp.bfloat16
        shapes = (state, state, state, jax.ShapeDtypeStruct((ITERS, 2), f32))
        packed = (2, PITCH, lanes)
        halo = (ITERS, 2, PITCH, lanes)
        parts = len(CHUNKS)
        results = pl.pallas_call(
            functools.partial(kernel, count, (pols, dirs, channels, width, pairs, entries)),
            out_shape=shapes,
            in_specs=[pl.BlockSpec(memory_space=pl.ANY)] * 4,
            out_specs=tuple([pl.BlockSpec(memory_space=pltpu.VMEM)] * 4),
            scratch_shapes=[
                pltpu.VMEM(visibility.shape, f32),
                pltpu.VMEM((tiles, 2, pols, dirs, channels, 128), bf16),
                pltpu.VMEM((2, pols, dirs, channels, pairs - 128 * whole), bf16),
                pltpu.VMEM(jones_start.shape, f32),
                pltpu.VMEM(duals_start.shape, f32),
                pltpu.VMEM((2, 2 * channels, tiles * 128), f32),
                pltpu.VMEM((2 * PITCH, 128), bf16),
                pltpu.VMEM((tiles, TALL, 128), bf16),
                pltpu.VMEM((2 * lanes, lanes), bf16),
                pltpu.VMEM((2, PITCH, PITCH, lanes), f32),
                pltpu.VMEM((2, PITCH, PITCH, lanes), f32),
                pltpu.VMEM((2, 2, GROUP, PITCH, lanes), f32),
                pltpu.VMEM((2, 2, GROUP, PITCH, lanes), f32),
                pltpu.VMEM((3, PITCH, lanes), f32),
                pltpu.VMEM((ITERS + 1,) + packed, f32),
                pltpu.VMEM(packed, f32),
                pltpu.VMEM(packed, f32),
                pltpu.VMEM(halo, f32),
                pltpu.VMEM(halo, f32),
                pltpu.VMEM(halo, f32),
                pltpu.VMEM((2 * ITERS, 8, lanes), f32),
                pltpu.VMEM((1, lanes), f32),
                pltpu.VMEM((count, 1, lanes), f32),
                pltpu.SemaphoreType.DMA((3,)),
                pltpu.SemaphoreType.DMA((whole,)),
                pltpu.SemaphoreType.DMA,
                pltpu.SemaphoreType.DMA((ITERS, parts, 2)),
                pltpu.SemaphoreType.DMA((ITERS, parts)),
                pltpu.SemaphoreType.DMA((ITERS, parts)),
                pltpu.SemaphoreType.DMA((count,)),
                pltpu.SemaphoreType.DMA((count,)),
            ],
            compiler_params=pltpu.CompilerParams(
                collective_id=0, has_side_effects=True, vmem_limit_bytes=24 * 1024 * 1024
            ),
        )(*[pltpu.with_memory_space_constraint(x, pltpu.HBM) for x in (visibility, sky, jones_start, duals_start)])
        return pl.pallas_call(
            deliver,
            out_shape=shapes,
            in_specs=[pl.BlockSpec(memory_space=pltpu.VMEM)] * 4,
            out_specs=tuple([pl.BlockSpec(memory_space=pl.ANY)] * 4),
            scratch_shapes=[pltpu.SemaphoreType.DMA((4,))],
            compiler_params=pltpu.CompilerParams(vmem_limit_bytes=4 * 1024 * 1024),
        )(*results)

    placed = (
        P(None, None, "chan", "slot", None),
        P(None, None, None, "chan", "slot", None),
        P(None, None, "slot", "chan", None),
        P(None, None, "slot", "chan", None),
    )
    return jax.shard_map(
        local,
        mesh=mesh,
        in_specs=placed,
        out_specs=(
            P(None, None, "slot", "chan", None),
            P(None, None, "slot", "chan", None),
            P(None, None, "slot", "chan", None),
            P("slot", None),
        ),
        check_vma=False,
    )
```

```python
import functools

import jax
import jax.numpy as jnp
from jax import lax
from jax.experimental import pallas as pl
from jax.experimental.pallas import tpu as pltpu
from jax.sharding import PartitionSpec as P

ITERS = 2
PITCH = 64
GROUP = 8
TALL = 144
HOLDS = (5, 7)
CHUNKS = ((0, 32), (32, 64))
MESH = pl.DeviceIdType.MESH

penalty = 8.0
kernel_taps = (0.04, 0.06, 0.1, 0.15, 0.3, 0.15, 0.1, 0.06, 0.04)


def kernel(
    count, dims,
    vis_in, sky_in, jones_in, duals_in,
    jones_out, consensus_out, duals_out, norms_out,
    vis_raw, sky_raw, tail_raw, jones_raw, duals_raw,
    vis_rows, chooser, placer, mixer, sky, vis, z_keep, rest, acc,
    gain, cons, dual, summed, from_low, from_high, sums, partial, slots,
    load_sem, sky_sem, tail_sem, send_sem, low_sem, high_sem, norm_send, norm_recv,
):
    pols, dirs, channels, width, pairs, entries = dims
    lanes = pols * dirs * channels
    tiles = pl.cdiv(pairs, 128)
    whole = pairs // 128
    me = lax.axis_index("chan")

    loads = [
        pltpu.make_async_copy(source, target, load_sem.at[i])
        for i, (source, target) in enumerate(((vis_in, vis_raw), (jones_in, jones_raw), (duals_in, duals_raw)))
    ]
    sky_rows = sky_in.reshape(2, pols, dirs * channels, pairs)
    sky_loads = [
        pltpu.make_async_copy(sky_rows.at[:, :, :, 128 * j : 128 * j + 128], sky_raw.at[j], sky_sem.at[j])
        for j in range(whole)
    ]
    tail_load = pltpu.make_async_copy(sky_rows.at[:, :, :, 128 * whole : pairs], tail_raw, tail_sem)
    for copy in loads:
        copy.start()

    def issue(j, carry):
        start = pl.multiple_of(j * 128, 128)
        pltpu.make_async_copy(sky_rows.at[:, :, :, pl.ds(start, 128)], sky_raw.at[j], sky_sem.at[j]).start()
        return carry

    lax.fori_loop(0, whole, issue, 0)
    tail_load.start()

    from_low[...] = jnp.zeros_like(from_low)
    from_high[...] = jnp.zeros_like(from_high)
    barrier = pltpu.get_barrier_semaphore()
    for step in range(1, count):
        pl.semaphore_signal(barrier, inc=1, device_id={"chan": lax.rem(me + step, count)}, device_id_type=MESH)
    sums[...] = jnp.zeros_like(sums)
    sky_raw[whole] = jnp.zeros(sky_raw.shape[1:], sky_raw.dtype)
    vis_rows[:, :, 128 * whole :] = jnp.zeros((2, 2 * channels, 128 * (tiles - whole)), jnp.float32)
    row = lax.broadcasted_iota(jnp.int32, (2 * PITCH, 128), 0)
    col = lax.broadcasted_iota(jnp.int32, (2 * PITCH, 128), 1)
    station = row & (PITCH - 1)
    target = jnp.where(row >= PITCH, station + width, station)
    chooser[...] = jnp.where((station < width) & (col == target), 1.0, 0.0).astype(jnp.bfloat16)
    def spot(pair):
        return pair + (PITCH - width) * (pair // width)

    bases = [spot(128 * j) // 8 * 8 for j in range(tiles)] + [width * PITCH]
    row = lax.broadcasted_iota(jnp.int32, (TALL, 128), 0).astype(jnp.float32)
    for j in range(tiles):
        pair = lax.broadcasted_iota(jnp.int32, (8, 128), 1).astype(jnp.float32) + 128.0 * j
        first = jnp.floor((pair + 0.5) * (1.0 / width))
        second = pair - first * width
        goal = pair + (PITCH - width) * first - bases[j]
        goal = jnp.where((first != second) & (first < width), goal, -1.0)
        placer[j] = jnp.where(row == goal[0:1], 1.0, 0.0).astype(jnp.bfloat16)
    row = lax.broadcasted_iota(jnp.int32, (2 * lanes, lanes), 0) & (lanes - 1)
    col = lax.broadcasted_iota(jnp.int32, (2 * lanes, lanes), 1)
    half = dirs * channels
    same = ((row >= half) == (col >= half)) & ((row & (channels - 1)) == (col & (channels - 1)))
    mixer[...] = jnp.where(same, -1.0, 0.0).astype(jnp.bfloat16)

    def window(first, second, i):
        offset = (2 * width * i) % 128
        if offset == 0:
            return first
        back = 128 - offset
        lane = lax.broadcasted_iota(jnp.int32, first.shape, 1)
        return jnp.where(lane < back, pltpu.roll(first, back, 1), pltpu.roll(second, back, 1))

    def swung(left, right):
        return lax.dot_general(left, right, (((1,), (1,)), ((), ())), preferred_element_type=jnp.float32)

    loads[0].wait()
    for part in range(2):
        for pol in range(pols):
            for f in range(channels):
                vis_rows[part, pol * channels + f : pol * channels + f + 1, 0:pairs] = vis_raw[part, pol, f]
    upper = lax.broadcasted_iota(jnp.int32, (2 * channels, 128), 0) < channels
    lane = lax.broadcasted_iota(jnp.int32, (2 * PITCH, lanes), 1)
    real = (lane & 8) == 0
    gap = jnp.zeros((half - 16, 128), jnp.float32)

    def vis_side(i):
        j = (2 * width * i) // 128
        first, second = [], []
        for part in range(2):
            value = window(vis_rows[part, :, 128 * j : 128 * j + 128], vis_rows[part, :, 128 * j + 128 : 128 * j + 256], i)
            high = value.astype(jnp.bfloat16).astype(jnp.float32)
            low = pltpu.roll(value - high, channels, 0)
            first.append(jnp.where(upper, high, low))
            second.append(jnp.where(upper, low, high))
        return jnp.concatenate(first + [gap] + second + [gap], 0).astype(jnp.bfloat16)

    for i in range(0, width // 2, 2):
        both = range(i, min(i + 2, width // 2))
        turned = swung(chooser[...], jnp.concatenate([vis_side(k) for k in both], 0))
        for n, k in enumerate(both):
            mine = turned[:, n * lanes : (n + 1) * lanes]
            vis[0, 2 * k : 2 * k + 2] = jnp.where(real, mine, 0.0).reshape(2, PITCH, lanes)
            vis[1, 2 * k : 2 * k + 2] = jnp.where(real, 0.0, mine).reshape(2, PITCH, lanes)

    for copy in loads[1:]:
        copy.wait()
    for part in range(2):
        start = jnp.transpose(jones_raw[part].reshape(lanes, width))
        gain[0, part, 0:width] = start
        cons[part, 0:width] = start
        dual[part, 0:width] = jnp.transpose(duals_raw[part].reshape(lanes, width))
        empty = jnp.zeros((PITCH - width, lanes), jnp.float32)
        gain[0, part, width:] = empty
        cons[part, width:] = empty
        dual[part, width:] = empty

    state = {"tile": 0, "left": None, "have": 0}

    def fetched(limit):
        while state["have"] < min(limit, tiles):
            if state["have"] < whole:
                sky_loads[state["have"]].wait()
            else:
                tail_load.wait()
                sky_raw[whole, :, :, :, 0 : pairs - 128 * whole] = tail_raw[...]
            state["have"] += 1

    flat = sky.reshape(2, PITCH * PITCH, lanes)

    def turn(limit):
        while state["tile"] < tiles and bases[state["tile"]] < limit:
            j = state["tile"]
            turned = swung(placer[j], sky_raw[j].reshape(2 * lanes, 128))
            size = bases[j + 1] - bases[j]
            left = []
            for part in range(2):
                mine = turned[:, part * lanes : (part + 1) * lanes]
                head = mine[0:8]
                if state["left"] is not None:
                    head = head + state["left"][part]
                flat[part, bases[j] : bases[j] + 8] = head
                if size > 8:
                    flat[part, bases[j] + 8 : bases[j + 1]] = mine[8:size]
                left.append(mine[size : size + 8] if size + 8 <= TALL else None)
            state["tile"], state["left"] = j + 1, left

    def parted(value):
        high = value.astype(jnp.bfloat16)
        low = (value - high.astype(jnp.float32)).astype(jnp.bfloat16)
        return jnp.concatenate([high, low], 1)

    def gathered_rows(values):
        row = lax.broadcasted_iota(jnp.int32, (8, lanes), 0)
        for bit in (1, 2, 4):
            even = (row & bit) == 0
            values = [
                jnp.where(even, a, b) + pltpu.roll(jnp.where(even, b, a), bit, 0)
                for a, b in zip(values[0::2], values[1::2])
            ]
        return values[0]

    def front(it, block):
        gr, gi = gain[it, 0], gain[it, 1]
        bank = block % 2
        sides = ([], [])
        here = min(GROUP, width - block * GROUP)
        for b in range(here):
            p = block * GROUP + b
            sr, si = sky[0, p], sky[1, p]
            zr = sr * gr + si * gi
            zi = sr * gi - si * gr
            z_keep[bank, 0, b] = zr
            z_keep[bank, 1, b] = zi
            lr, li = gain[it, 0, p : p + 1], gain[it, 1, p : p + 1]
            sides[0].append(parted(lr * zr + li * zi - vis[0, p]))
            sides[1].append(parted(li * zr - lr * zi - vis[1, p]))
        for part in range(2):
            rest[bank, part, 0:here] = jnp.dot(
                jnp.concatenate(sides[part], 0), mixer[...], preferred_element_type=jnp.float32
            ).reshape(here, PITCH, lanes)

    def back(block):
        bank = block % 2
        sums_of = [[], [], []]
        for b in range(min(GROUP, width - block * GROUP)):
            zr, zi = z_keep[bank, 0, b], z_keep[bank, 1, b]
            dr, di = rest[bank, 0, b], rest[bank, 1, b]
            for i, value in enumerate((dr * zr - di * zi, dr * zi + di * zr, zr * zr + zi * zi)):
                sums_of[i].append(jnp.sum(value.reshape(PITCH // 8, 8, lanes), 0))
        for i in range(3):
            sums_of[i] += [jnp.zeros((8, lanes), jnp.float32)] * (GROUP - len(sums_of[i]))
            acc[i, block * GROUP : (block + 1) * GROUP] = gathered_rows(sums_of[i])

    place = lax.broadcasted_iota(jnp.int32, (8, lanes), 1) & (channels - 1)

    def mixed(block, distance):
        out = None
        for shift in range(1 - channels, channels):
            offset = distance + shift + 4
            if offset < 0 or offset > 8:
                continue
            inside = (place + shift >= 0) & (place + shift < channels)
            weight = jnp.where(inside, kernel_taps[offset], 0.0)[0:1]
            moved = block if shift == 0 else pltpu.roll(block, (-shift) % lanes, 1)
            term = weight * moved
            out = term if out is None else out + term
        return out

    def up_copy(it, chunk):
        return pltpu.make_async_remote_copy(
            src_ref=summed.at[it, :, slice(*CHUNKS[chunk])], dst_ref=from_low.at[it, :, slice(*CHUNKS[chunk])],
            send_sem=send_sem.at[it, chunk, 0], recv_sem=low_sem.at[it, chunk],
            device_id={"chan": lax.rem(me + 1, count)}, device_id_type=MESH,
        )

    def down_copy(it, chunk):
        return pltpu.make_async_remote_copy(
            src_ref=summed.at[it, :, slice(*CHUNKS[chunk])], dst_ref=from_high.at[it, :, slice(*CHUNKS[chunk])],
            send_sem=send_sem.at[it, chunk, 1], recv_sem=high_sem.at[it, chunk],
            device_id={"chan": lax.rem(me + count - 1, count)}, device_id_type=MESH,
        )

    def finish(it, chunk):
        rows = slice(*CHUNKS[chunk])
        lower = acc[2, rows]
        scale = lower + penalty
        for part in range(2):
            goal = cons[part, rows] - dual[part, rows]
            fresh = (acc[part, rows] + gain[it, part, rows] * lower + penalty * goal) / scale
            gain[it + 1, part, rows] = fresh
            summed[it, part, rows] = fresh + dual[part, rows]

        @pl.when(me < count - 1)
        def _():
            up_copy(it, chunk).start()

        @pl.when(me > 0)
        def _():
            down_copy(it, chunk).start()

    def smooth(it, chunk):
        rows = slice(*CHUNKS[chunk])

        @pl.when(me > 0)
        def _():
            up_copy(it, chunk).wait_recv()

        @pl.when(me < count - 1)
        def _():
            down_copy(it, chunk).wait_recv()

        for part in range(2):
            fresh = (
                mixed(summed[it, part, rows], 0)
                + mixed(from_low[it, part, rows], -channels)
                + mixed(from_high[it, part, rows], channels)
            )
            off = gain[it + 1, part, rows] - fresh
            moved = fresh - cons[part, rows]
            dual[part, rows] = dual[part, rows] + off
            cons[part, rows] = fresh
            sums[2 * it] += jnp.sum((off * off).reshape(-1, 8, lanes), 0)
            sums[2 * it + 1] += jnp.sum((moved * moved).reshape(-1, 8, lanes), 0)

    def norm_copy(step):
        return pltpu.make_async_remote_copy(
            src_ref=partial, dst_ref=slots.at[me],
            send_sem=norm_send.at[step], recv_sem=norm_recv.at[step],
            device_id={"chan": lax.rem(me + step, count)}, device_id_type=MESH,
        )

    def put(target, state):
        for part in range(2):
            target[part] = jnp.transpose(state[part])[:, 0:width].reshape(pols, dirs, channels, width)

    blocks = PITCH // GROUP
    stops = {stop // GROUP - 1: chunk for chunk, (_, stop) in enumerate(CHUNKS)}
    fetched(tiles)
    turn(GROUP * PITCH)
    for it in range(ITERS):
        front(it, 0)
        for block in range(blocks):
            if it == 0:
                turn((block + 2) * GROUP * PITCH)
            if block + 1 < blocks:
                front(it, block + 1)
            back(block)
            if it == 0 and block in stops:
                if stops[block] == 0:
                    pl.semaphore_wait(barrier, count - 1)
                finish(it, stops[block])
            if it > 0:
                for chunk, hold in enumerate(HOLDS):
                    if block == hold:
                        smooth(it - 1, chunk)
                        finish(it, chunk)
    put(jones_out, gain.at[ITERS])
    for chunk in range(len(CHUNKS)):
        smooth(ITERS - 1, chunk)

    lane = lax.broadcasted_iota(jnp.int32, (1, lanes), 1)
    share = lanes // (2 * ITERS)
    packed = jnp.zeros((1, lanes), jnp.float32)
    for i in range(2 * ITERS):
        value = jnp.sum(sums[i], 0, keepdims=True)
        stride = lanes // 2
        while stride >= share:
            value = value + pltpu.roll(value, stride, 1)
            stride //= 2
        packed = jnp.where(lane // share == i, value, packed)
    partial[...] = packed
    slots[pl.ds(me, 1)] = packed[None]
    for step in range(1, count):
        norm_copy(step).start()
    put(consensus_out, cons)
    put(duals_out, dual)

    for it in range(ITERS):
        for chunk in range(len(CHUNKS)):

            @pl.when(me < count - 1)
            def _():
                up_copy(it, chunk).wait_send()

            @pl.when(me > 0)
            def _():
                down_copy(it, chunk).wait_send()

    for step in range(1, count):
        norm_copy(step).wait()
    gathered = slots[0]
    for j in range(1, count):
        gathered = gathered + slots[j]
    for it in range(ITERS):
        for n, factor in enumerate((1.0, penalty * penalty)):
            mine = jnp.where(lane // share == 2 * it + n, gathered, 0.0)
            norms_out[it : it + 1, n : n + 1] = jnp.sum(mine, axis=1, keepdims=True) * (factor / entries)


def deliver(*refs):
    sources, targets, sem = refs[0:4], refs[4:8], refs[8]
    copies = [pltpu.make_async_copy(s, t, sem.at[i]) for i, (s, t) in enumerate(zip(sources, targets))]
    for copy in copies:
        copy.start()
    for copy in copies:
        copy.wait()


def solution(mesh):
    count = mesh.shape["chan"]

    def local(visibility, coherency, jones_start, duals_start):
        _, pols, dirs, channels, width = jones_start.shape
        pairs = visibility.shape[-1]
        times = visibility.shape[3]
        lanes = pols * dirs * channels
        assert times == 1 and pols == 2 and channels == 4 and lanes == 128 and width <= PITCH - 2 and width % 2 == 0
        tiles = pl.cdiv(pairs, 128)
        whole = pairs // 128
        entries = jones_start.size * count
        sky = coherency.transpose(0, 1, 2, 4, 3, 5).reshape(2, pols, dirs, channels, pairs)
        state = jax.ShapeDtypeStruct(jones_start.shape, jnp.float32)
        f32, bf16 = jnp.float32, jnp.bfloat16
        shapes = (state, state, state, jax.ShapeDtypeStruct((ITERS, 2), f32))
        packed = (2, PITCH, lanes)
        halo = (ITERS, 2, PITCH, lanes)
        parts = len(CHUNKS)
        results = pl.pallas_call(
            functools.partial(kernel, count, (pols, dirs, channels, width, pairs, entries)),
            out_shape=shapes,
            in_specs=[pl.BlockSpec(memory_space=pl.ANY)] * 4,
            out_specs=tuple([pl.BlockSpec(memory_space=pltpu.VMEM)] * 4),
            scratch_shapes=[
                pltpu.VMEM(visibility.shape, f32),
                pltpu.VMEM((tiles, 2, pols, dirs * channels, 128), bf16),
                pltpu.VMEM((2, pols, dirs * channels, pairs - 128 * whole), bf16),
                pltpu.VMEM(jones_start.shape, f32),
                pltpu.VMEM(duals_start.shape, f32),
                pltpu.VMEM((2, 2 * channels, tiles * 128), f32),
                pltpu.VMEM((2 * PITCH, 128), bf16),
                pltpu.VMEM((tiles, TALL, 128), bf16),
                pltpu.VMEM((2 * lanes, lanes), bf16),
                pltpu.VMEM((2, PITCH, PITCH, lanes), f32),
                pltpu.VMEM((2, PITCH, PITCH, lanes), f32),
                pltpu.VMEM((2, 2, GROUP, PITCH, lanes), f32),
                pltpu.VMEM((2, 2, GROUP, PITCH, lanes), f32),
                pltpu.VMEM((3, PITCH, lanes), f32),
                pltpu.VMEM((ITERS + 1,) + packed, f32),
                pltpu.VMEM(packed, f32),
                pltpu.VMEM(packed, f32),
                pltpu.VMEM(halo, f32),
                pltpu.VMEM(halo, f32),
                pltpu.VMEM(halo, f32),
                pltpu.VMEM((2 * ITERS, 8, lanes), f32),
                pltpu.VMEM((1, lanes), f32),
                pltpu.VMEM((count, 1, lanes), f32),
                pltpu.SemaphoreType.DMA((3,)),
                pltpu.SemaphoreType.DMA((whole,)),
                pltpu.SemaphoreType.DMA,
                pltpu.SemaphoreType.DMA((ITERS, parts, 2)),
                pltpu.SemaphoreType.DMA((ITERS, parts)),
                pltpu.SemaphoreType.DMA((ITERS, parts)),
                pltpu.SemaphoreType.DMA((count,)),
                pltpu.SemaphoreType.DMA((count,)),
            ],
            compiler_params=pltpu.CompilerParams(
                collective_id=0, has_side_effects=True, vmem_limit_bytes=24 * 1024 * 1024
            ),
        )(*[pltpu.with_memory_space_constraint(x, pltpu.HBM) for x in (visibility, sky, jones_start, duals_start)])
        return pl.pallas_call(
            deliver,
            out_shape=shapes,
            in_specs=[pl.BlockSpec(memory_space=pltpu.VMEM)] * 4,
            out_specs=tuple([pl.BlockSpec(memory_space=pl.ANY)] * 4),
            scratch_shapes=[pltpu.SemaphoreType.DMA((4,))],
            compiler_params=pltpu.CompilerParams(vmem_limit_bytes=4 * 1024 * 1024),
        )(*results)

    placed = (
        P(None, None, "chan", "slot", None),
        P(None, None, None, "chan", "slot", None),
        P(None, None, "slot", "chan", None),
        P(None, None, "slot", "chan", None),
    )
    return jax.shard_map(
        local,
        mesh=mesh,
        in_specs=placed,
        out_specs=(
            P(None, None, "slot", "chan", None),
            P(None, None, "slot", "chan", None),
            P(None, None, "slot", "chan", None),
            P("slot", None),
        ),
        check_vma=False,
    )
```

```python
import functools

import jax
import jax.numpy as jnp
from jax import lax
from jax.experimental import pallas as pl
from jax.experimental.pallas import tpu as pltpu
from jax.sharding import PartitionSpec as P

ITERS = 2
PITCH = 64
GROUP = 8
TALL = 144
HOLDS = (5, 7)
CHUNKS = ((0, 32), (32, 64))
MESH = pl.DeviceIdType.MESH

penalty = 8.0
kernel_taps = (0.04, 0.06, 0.1, 0.15, 0.3, 0.15, 0.1, 0.06, 0.04)


def kernel(
    count, dims,
    vis_in, sky_in, jones_in, duals_in,
    jones_out, consensus_out, duals_out, norms_out,
    vis_raw, sky_raw, tail_raw, jones_raw, duals_raw,
    vis_rows, chooser, placer, mixer, sky, vis, z_keep, rest, acc,
    gain, cons, dual, summed, from_low, from_high, sums, partial, slots,
    load_sem, sky_sem, tail_sem, send_sem, low_sem, high_sem, norm_send, norm_recv,
):
    pols, dirs, channels, width, pairs, entries = dims
    lanes = pols * dirs * channels
    tiles = pl.cdiv(pairs, 128)
    whole = pairs // 128
    me = lax.axis_index("chan")

    loads = [
        pltpu.make_async_copy(source, target, load_sem.at[i])
        for i, (source, target) in enumerate(((vis_in, vis_raw), (jones_in, jones_raw), (duals_in, duals_raw)))
    ]
    sky_rows = sky_in.reshape(2, pols, dirs * channels, pairs)
    sky_loads = [
        pltpu.make_async_copy(sky_rows.at[:, :, :, 128 * j : 128 * j + 128], sky_raw.at[j], sky_sem.at[j])
        for j in range(whole)
    ]
    tail_load = pltpu.make_async_copy(sky_rows.at[:, :, :, 128 * whole : pairs], tail_raw, tail_sem)
    for copy in loads:
        copy.start()

    def issue(j, carry):
        start = pl.multiple_of(j * 128, 128)
        pltpu.make_async_copy(sky_rows.at[:, :, :, pl.ds(start, 128)], sky_raw.at[j], sky_sem.at[j]).start()
        return carry

    lax.fori_loop(0, whole, issue, 0)
    tail_load.start()

    from_low[...] = jnp.zeros_like(from_low)
    from_high[...] = jnp.zeros_like(from_high)
    barrier = pltpu.get_barrier_semaphore()
    for step in range(1, count):
        pl.semaphore_signal(barrier, inc=1, device_id={"chan": lax.rem(me + step, count)}, device_id_type=MESH)
    sums[...] = jnp.zeros_like(sums)
    sky_raw[whole] = jnp.zeros(sky_raw.shape[1:], sky_raw.dtype)
    vis_rows[:, :, 128 * whole :] = jnp.zeros((2, 2 * channels, 128 * (tiles - whole)), jnp.float32)
    row = lax.broadcasted_iota(jnp.int32, (2 * PITCH, 128), 0)
    col = lax.broadcasted_iota(jnp.int32, (2 * PITCH, 128), 1)
    station = row & (PITCH - 1)
    target = jnp.where(row >= PITCH, station + width, station)
    chooser[...] = jnp.where((station < width) & (col == target), 1.0, 0.0).astype(jnp.bfloat16)
    def spot(pair):
        return pair + (PITCH - width) * (pair // width)

    bases = [spot(128 * j) // 8 * 8 for j in range(tiles)] + [width * PITCH]
    row = lax.broadcasted_iota(jnp.int32, (TALL, 128), 0).astype(jnp.float32)
    for j in range(tiles):
        pair = lax.broadcasted_iota(jnp.int32, (8, 128), 1).astype(jnp.float32) + 128.0 * j
        first = jnp.floor((pair + 0.5) * (1.0 / width))
        second = pair - first * width
        goal = pair + (PITCH - width) * first - bases[j]
        goal = jnp.where((first != second) & (first < width), goal, -1.0)
        placer[j] = jnp.where(row == goal[0:1], 1.0, 0.0).astype(jnp.bfloat16)
    row = lax.broadcasted_iota(jnp.int32, (2 * lanes, lanes), 0) & (lanes - 1)
    col = lax.broadcasted_iota(jnp.int32, (2 * lanes, lanes), 1)
    half = dirs * channels
    same = ((row >= half) == (col >= half)) & ((row & (channels - 1)) == (col & (channels - 1)))
    mixer[...] = jnp.where(same, -1.0, 0.0).astype(jnp.bfloat16)

    def window(first, second, i):
        offset = (2 * width * i) % 128
        if offset == 0:
            return first
        back = 128 - offset
        lane = lax.broadcasted_iota(jnp.int32, first.shape, 1)
        return jnp.where(lane < back, pltpu.roll(first, back, 1), pltpu.roll(second, back, 1))

    def swung(left, right):
        return lax.dot_general(left, right, (((1,), (1,)), ((), ())), preferred_element_type=jnp.float32)

    loads[0].wait()
    for part in range(2):
        for pol in range(pols):
            for f in range(channels):
                vis_rows[part, pol * channels + f : pol * channels + f + 1, 0:pairs] = vis_raw[part, pol, f]
    upper = lax.broadcasted_iota(jnp.int32, (2 * channels, 128), 0) < channels
    lane = lax.broadcasted_iota(jnp.int32, (2 * PITCH, lanes), 1)
    real = (lane & 8) == 0
    gap = jnp.zeros((half - 16, 128), jnp.float32)

    def vis_side(i):
        j = (2 * width * i) // 128
        first, second = [], []
        for part in range(2):
            value = window(vis_rows[part, :, 128 * j : 128 * j + 128], vis_rows[part, :, 128 * j + 128 : 128 * j + 256], i)
            high = value.astype(jnp.bfloat16).astype(jnp.float32)
            low = pltpu.roll(value - high, channels, 0)
            first.append(jnp.where(upper, high, low))
            second.append(jnp.where(upper, low, high))
        return jnp.concatenate(first + [gap] + second + [gap], 0).astype(jnp.bfloat16)

    for i in range(0, width // 2, 2):
        both = range(i, min(i + 2, width // 2))
        turned = swung(chooser[...], jnp.concatenate([vis_side(k) for k in both], 0))
        for n, k in enumerate(both):
            mine = turned[:, n * lanes : (n + 1) * lanes]
            vis[0, 2 * k : 2 * k + 2] = jnp.where(real, mine, 0.0).reshape(2, PITCH, lanes)
            vis[1, 2 * k : 2 * k + 2] = jnp.where(real, 0.0, mine).reshape(2, PITCH, lanes)

    for copy in loads[1:]:
        copy.wait()
    for part in range(2):
        start = jnp.transpose(jones_raw[part].reshape(lanes, width))
        gain[0, part, 0:width] = start
        cons[part, 0:width] = start
        dual[part, 0:width] = jnp.transpose(duals_raw[part].reshape(lanes, width))
        empty = jnp.zeros((PITCH - width, lanes), jnp.float32)
        gain[0, part, width:] = empty
        cons[part, width:] = empty
        dual[part, width:] = empty

    state = {"tile": 0, "left": None, "have": 0}

    def fetched(limit):
        while state["have"] < min(limit, tiles):
            if state["have"] < whole:
                sky_loads[state["have"]].wait()
            else:
                tail_load.wait()
                sky_raw[whole, :, :, :, 0 : pairs - 128 * whole] = tail_raw[...]
            state["have"] += 1

    flat = sky.reshape(2, PITCH * PITCH, lanes)

    def turn(limit):
        while state["tile"] < tiles and bases[state["tile"]] < limit:
            j = state["tile"]
            turned = swung(placer[j], sky_raw[j].reshape(2 * lanes, 128))
            size = bases[j + 1] - bases[j]
            left = []
            for part in range(2):
                mine = turned[:, part * lanes : (part + 1) * lanes]
                head = mine[0:8]
                if state["left"] is not None:
                    head = head + state["left"][part]
                flat[part, bases[j] : bases[j] + 8] = head
                if size > 8:
                    flat[part, bases[j] + 8 : bases[j + 1]] = mine[8:size]
                left.append(mine[size : size + 8] if size + 8 <= TALL else None)
            state["tile"], state["left"] = j + 1, left

    def parted(value):
        high = value.astype(jnp.bfloat16)
        low = (value - high.astype(jnp.float32)).astype(jnp.bfloat16)
        return jnp.concatenate([high, low], 1)

    def gathered_rows(values):
        row = lax.broadcasted_iota(jnp.int32, (8, lanes), 0)
        for bit in (1, 2, 4):
            even = (row & bit) == 0
            values = [
                jnp.where(even, a, b) + pltpu.roll(jnp.where(even, b, a), bit, 0)
                for a, b in zip(values[0::2], values[1::2])
            ]
        return values[0]

    def front(it, block):
        gr, gi = gain[it, 0], gain[it, 1]
        bank = block % 2
        sides = ([], [])
        here = min(GROUP, width - block * GROUP)
        for b in range(here):
            p = block * GROUP + b
            sr, si = sky[0, p], sky[1, p]
            zr = sr * gr + si * gi
            zi = sr * gi - si * gr
            z_keep[bank, 0, b] = zr
            z_keep[bank, 1, b] = zi
            lr, li = gain[it, 0, p : p + 1], gain[it, 1, p : p + 1]
            sides[0].append(parted(lr * zr + li * zi - vis[0, p]))
            sides[1].append(parted(li * zr - lr * zi - vis[1, p]))
        for part in range(2):
            rest[bank, part, 0:here] = jnp.dot(
                jnp.concatenate(sides[part], 0), mixer[...], preferred_element_type=jnp.float32
            ).reshape(here, PITCH, lanes)

    def back(block):
        bank = block % 2
        sums_of = [[], [], []]
        for b in range(min(GROUP, width - block * GROUP)):
            zr, zi = z_keep[bank, 0, b], z_keep[bank, 1, b]
            dr, di = rest[bank, 0, b], rest[bank, 1, b]
            for i, value in enumerate((dr * zr - di * zi, dr * zi + di * zr, zr * zr + zi * zi)):
                sums_of[i].append(jnp.sum(value.reshape(PITCH // 8, 8, lanes), 0))
        for i in range(3):
            sums_of[i] += [jnp.zeros((8, lanes), jnp.float32)] * (GROUP - len(sums_of[i]))
            acc[i, block * GROUP : (block + 1) * GROUP] = gathered_rows(sums_of[i])

    place = lax.broadcasted_iota(jnp.int32, (8, lanes), 1) & (channels - 1)

    def mixed(block, distance):
        out = None
        for shift in range(1 - channels, channels):
            offset = distance + shift + 4
            if offset < 0 or offset > 8:
                continue
            inside = (place + shift >= 0) & (place + shift < channels)
            weight = jnp.where(inside, kernel_taps[offset], 0.0)[0:1]
            moved = block if shift == 0 else pltpu.roll(block, (-shift) % lanes, 1)
            term = weight * moved
            out = term if out is None else out + term
        return out

    def up_copy(it, chunk):
        return pltpu.make_async_remote_copy(
            src_ref=summed.at[it, :, slice(*CHUNKS[chunk])], dst_ref=from_low.at[it, :, slice(*CHUNKS[chunk])],
            send_sem=send_sem.at[it, chunk, 0], recv_sem=low_sem.at[it, chunk],
            device_id={"chan": lax.rem(me + 1, count)}, device_id_type=MESH,
        )

    def down_copy(it, chunk):
        return pltpu.make_async_remote_copy(
            src_ref=summed.at[it, :, slice(*CHUNKS[chunk])], dst_ref=from_high.at[it, :, slice(*CHUNKS[chunk])],
            send_sem=send_sem.at[it, chunk, 1], recv_sem=high_sem.at[it, chunk],
            device_id={"chan": lax.rem(me + count - 1, count)}, device_id_type=MESH,
        )

    def finish(it, chunk):
        rows = slice(*CHUNKS[chunk])
        lower = acc[2, rows]
        scale = 1.0 / (lower + penalty)
        for part in range(2):
            goal = cons[part, rows] - dual[part, rows]
            fresh = (acc[part, rows] + gain[it, part, rows] * lower + penalty * goal) * scale
            gain[it + 1, part, rows] = fresh
            summed[it, part, rows] = fresh + dual[part, rows]

        @pl.when(me < count - 1)
        def _():
            up_copy(it, chunk).start()

        @pl.when(me > 0)
        def _():
            down_copy(it, chunk).start()

    def smooth(it, chunk):
        rows = slice(*CHUNKS[chunk])
        own = [mixed(summed[it, part, rows], 0) for part in range(2)]

        @pl.when(me > 0)
        def _():
            up_copy(it, chunk).wait_recv()

        @pl.when(me < count - 1)
        def _():
            down_copy(it, chunk).wait_recv()

        for part in range(2):
            fresh = (
                own[part]
                + mixed(from_low[it, part, rows], -channels)
                + mixed(from_high[it, part, rows], channels)
            )
            off = gain[it + 1, part, rows] - fresh
            moved = fresh - cons[part, rows]
            dual[part, rows] = dual[part, rows] + off
            cons[part, rows] = fresh
            sums[2 * it] += jnp.sum((off * off).reshape(-1, 8, lanes), 0)
            sums[2 * it + 1] += jnp.sum((moved * moved).reshape(-1, 8, lanes), 0)

    def norm_copy(step):
        return pltpu.make_async_remote_copy(
            src_ref=partial, dst_ref=slots.at[me],
            send_sem=norm_send.at[step], recv_sem=norm_recv.at[step],
            device_id={"chan": lax.rem(me + step, count)}, device_id_type=MESH,
        )

    def put(target, state):
        for part in range(2):
            target[part] = jnp.transpose(state[part])[:, 0:width].reshape(pols, dirs, channels, width)

    blocks = PITCH // GROUP
    stops = {stop // GROUP - 1: chunk for chunk, (_, stop) in enumerate(CHUNKS)}
    fetched(10)
    turn(2 * GROUP * PITCH)
    fetched(tiles)
    for it in range(ITERS):
        front(it, 0)
        for block in range(blocks):
            if it == 0:
                turn((block + 2) * GROUP * PITCH)
            if block + 1 < blocks:
                front(it, block + 1)
            back(block)
            if it == 0 and block in stops:
                if stops[block] == 0:
                    pl.semaphore_wait(barrier, count - 1)
                finish(it, stops[block])
            if it > 0:
                for chunk, hold in enumerate(HOLDS):
                    if block == hold:
                        smooth(it - 1, chunk)
                        finish(it, chunk)
    put(jones_out, gain.at[ITERS])
    for chunk in range(len(CHUNKS)):
        smooth(ITERS - 1, chunk)

    lane = lax.broadcasted_iota(jnp.int32, (1, lanes), 1)
    share = lanes // (2 * ITERS)
    packed = jnp.zeros((1, lanes), jnp.float32)
    for i in range(2 * ITERS):
        value = jnp.sum(sums[i], 0, keepdims=True)
        stride = lanes // 2
        while stride >= share:
            value = value + pltpu.roll(value, stride, 1)
            stride //= 2
        packed = jnp.where(lane // share == i, value, packed)
    partial[...] = packed
    slots[pl.ds(me, 1)] = packed[None]
    for step in range(1, count):
        norm_copy(step).start()
    put(consensus_out, cons)
    put(duals_out, dual)

    for it in range(ITERS):
        for chunk in range(len(CHUNKS)):

            @pl.when(me < count - 1)
            def _():
                up_copy(it, chunk).wait_send()

            @pl.when(me > 0)
            def _():
                down_copy(it, chunk).wait_send()

    for step in range(1, count):
        norm_copy(step).wait_send()
    for step in range(1, count):
        norm_copy(step).wait_recv()
    gathered = slots[0]
    for j in range(1, count):
        gathered = gathered + slots[j]
    for it in range(ITERS):
        for n, factor in enumerate((1.0, penalty * penalty)):
            mine = jnp.where(lane // share == 2 * it + n, gathered, 0.0)
            norms_out[it : it + 1, n : n + 1] = jnp.sum(mine, axis=1, keepdims=True) * (factor / entries)


def deliver(*refs):
    sources, targets, sem = refs[0:4], refs[4:8], refs[8]
    copies = [pltpu.make_async_copy(s, t, sem.at[i]) for i, (s, t) in enumerate(zip(sources, targets))]
    for copy in copies:
        copy.start()
    for copy in copies:
        copy.wait()


def solution(mesh):
    count = mesh.shape["chan"]

    def local(visibility, coherency, jones_start, duals_start):
        _, pols, dirs, channels, width = jones_start.shape
        pairs = visibility.shape[-1]
        times = visibility.shape[3]
        lanes = pols * dirs * channels
        assert times == 1 and pols == 2 and channels == 4 and lanes == 128 and width <= PITCH - 2 and width % 2 == 0
        tiles = pl.cdiv(pairs, 128)
        whole = pairs // 128
        entries = jones_start.size * count
        sky = coherency.transpose(0, 1, 2, 4, 3, 5).reshape(2, pols, dirs, channels, pairs)
        state = jax.ShapeDtypeStruct(jones_start.shape, jnp.float32)
        f32, bf16 = jnp.float32, jnp.bfloat16
        shapes = (state, state, state, jax.ShapeDtypeStruct((ITERS, 2), f32))
        packed = (2, PITCH, lanes)
        halo = (ITERS, 2, PITCH, lanes)
        parts = len(CHUNKS)
        results = pl.pallas_call(
            functools.partial(kernel, count, (pols, dirs, channels, width, pairs, entries)),
            out_shape=shapes,
            in_specs=[pl.BlockSpec(memory_space=pl.ANY)] * 4,
            out_specs=tuple([pl.BlockSpec(memory_space=pltpu.VMEM)] * 4),
            scratch_shapes=[
                pltpu.VMEM(visibility.shape, f32),
                pltpu.VMEM((tiles, 2, pols, dirs * channels, 128), bf16),
                pltpu.VMEM((2, pols, dirs * channels, pairs - 128 * whole), bf16),
                pltpu.VMEM(jones_start.shape, f32),
                pltpu.VMEM(duals_start.shape, f32),
                pltpu.VMEM((2, 2 * channels, tiles * 128), f32),
                pltpu.VMEM((2 * PITCH, 128), bf16),
                pltpu.VMEM((tiles, TALL, 128), bf16),
                pltpu.VMEM((2 * lanes, lanes), bf16),
                pltpu.VMEM((2, PITCH, PITCH, lanes), f32),
                pltpu.VMEM((2, PITCH, PITCH, lanes), f32),
                pltpu.VMEM((2, 2, GROUP, PITCH, lanes), f32),
                pltpu.VMEM((2, 2, GROUP, PITCH, lanes), f32),
                pltpu.VMEM((3, PITCH, lanes), f32),
                pltpu.VMEM((ITERS + 1,) + packed, f32),
                pltpu.VMEM(packed, f32),
                pltpu.VMEM(packed, f32),
                pltpu.VMEM(halo, f32),
                pltpu.VMEM(halo, f32),
                pltpu.VMEM(halo, f32),
                pltpu.VMEM((2 * ITERS, 8, lanes), f32),
                pltpu.VMEM((1, lanes), f32),
                pltpu.VMEM((count, 1, lanes), f32),
                pltpu.SemaphoreType.DMA((3,)),
                pltpu.SemaphoreType.DMA((whole,)),
                pltpu.SemaphoreType.DMA,
                pltpu.SemaphoreType.DMA((ITERS, parts, 2)),
                pltpu.SemaphoreType.DMA((ITERS, parts)),
                pltpu.SemaphoreType.DMA((ITERS, parts)),
                pltpu.SemaphoreType.DMA((count,)),
                pltpu.SemaphoreType.DMA((count,)),
            ],
            compiler_params=pltpu.CompilerParams(
                collective_id=0, has_side_effects=True, vmem_limit_bytes=24 * 1024 * 1024
            ),
        )(*[pltpu.with_memory_space_constraint(x, pltpu.HBM) for x in (visibility, sky, jones_start, duals_start)])
        return pl.pallas_call(
            deliver,
            out_shape=shapes,
            in_specs=[pl.BlockSpec(memory_space=pltpu.VMEM)] * 4,
            out_specs=tuple([pl.BlockSpec(memory_space=pl.ANY)] * 4),
            scratch_shapes=[pltpu.SemaphoreType.DMA((4,))],
            compiler_params=pltpu.CompilerParams(vmem_limit_bytes=4 * 1024 * 1024),
        )(*results)

    placed = (
        P(None, None, "chan", "slot", None),
        P(None, None, None, "chan", "slot", None),
        P(None, None, "slot", "chan", None),
        P(None, None, "slot", "chan", None),
    )
    return jax.shard_map(
        local,
        mesh=mesh,
        in_specs=placed,
        out_specs=(
            P(None, None, "slot", "chan", None),
            P(None, None, "slot", "chan", None),
            P(None, None, "slot", "chan", None),
            P("slot", None),
        ),
        check_vma=False,
    )
```

```python
import functools

import jax
import jax.numpy as jnp
from jax import lax
from jax.experimental import pallas as pl
from jax.experimental.pallas import tpu as pltpu
from jax.sharding import PartitionSpec as P

ITERS = 2
PITCH = 64
GROUP = 8
TALL = 144
HOLDS = (5, 7)
CHUNKS = ((0, 32), (32, 64))
MESH = pl.DeviceIdType.MESH

penalty = 8.0
kernel_taps = (0.04, 0.06, 0.1, 0.15, 0.3, 0.15, 0.1, 0.06, 0.04)


def kernel(
    count, dims,
    vis_in, sky_in, jones_in, duals_in,
    jones_out, consensus_out, duals_out, norms_out,
    vis_raw, sky_raw, tail_raw, jones_raw, duals_raw,
    vis_rows, chooser, placer, mixer, sky, vis, z_keep, rest, acc,
    gain, cons, dual, summed, from_low, from_high, sums, partial, slots,
    load_sem, sky_sem, tail_sem, send_sem, low_sem, high_sem, norm_send, norm_recv,
):
    pols, dirs, channels, width, pairs, entries = dims
    lanes = pols * dirs * channels
    tiles = pl.cdiv(pairs, 128)
    whole = pairs // 128
    me = lax.axis_index("chan")

    loads = [
        pltpu.make_async_copy(source, target, load_sem.at[i])
        for i, (source, target) in enumerate(((vis_in, vis_raw), (jones_in, jones_raw), (duals_in, duals_raw)))
    ]
    sky_rows = sky_in.reshape(2, pols, dirs * channels, pairs)
    sky_loads = [
        pltpu.make_async_copy(sky_rows.at[:, :, :, 128 * j : 128 * j + 128], sky_raw.at[j], sky_sem.at[j])
        for j in range(whole)
    ]
    tail_load = pltpu.make_async_copy(sky_rows.at[:, :, :, 128 * whole : pairs], tail_raw, tail_sem)
    for copy in loads:
        copy.start()

    def issue(j, carry):
        start = pl.multiple_of(j * 128, 128)
        pltpu.make_async_copy(sky_rows.at[:, :, :, pl.ds(start, 128)], sky_raw.at[j], sky_sem.at[j]).start()
        return carry

    lax.fori_loop(0, whole, issue, 0)
    tail_load.start()

    from_low[...] = jnp.zeros_like(from_low)
    from_high[...] = jnp.zeros_like(from_high)
    barrier = pltpu.get_barrier_semaphore()
    for step in range(1, count):
        pl.semaphore_signal(barrier, inc=1, device_id={"chan": lax.rem(me + step, count)}, device_id_type=MESH)
    sums[...] = jnp.zeros_like(sums)
    sky_raw[whole] = jnp.zeros(sky_raw.shape[1:], sky_raw.dtype)
    vis_rows[:, :, 128 * whole :] = jnp.zeros((2, 2 * channels, 128 * (tiles - whole)), jnp.float32)
    row = lax.broadcasted_iota(jnp.int32, (2 * PITCH, 128), 0)
    col = lax.broadcasted_iota(jnp.int32, (2 * PITCH, 128), 1)
    station = row & (PITCH - 1)
    target = jnp.where(row >= PITCH, station + width, station)
    chooser[...] = jnp.where((station < width) & (col == target), 1.0, 0.0).astype(jnp.bfloat16)
    def spot(pair):
        return pair + (PITCH - width) * (pair // width)

    bases = [spot(128 * j) // 8 * 8 for j in range(tiles)] + [width * PITCH]
    row = lax.broadcasted_iota(jnp.int32, (TALL, 128), 0).astype(jnp.float32)
    for j in range(tiles):
        pair = lax.broadcasted_iota(jnp.int32, (8, 128), 1).astype(jnp.float32) + 128.0 * j
        first = jnp.floor((pair + 0.5) * (1.0 / width))
        second = pair - first * width
        goal = pair + (PITCH - width) * first - bases[j]
        goal = jnp.where((first != second) & (first < width), goal, -1.0)
        placer[j] = jnp.where(row == goal[0:1], 1.0, 0.0).astype(jnp.bfloat16)
    row = lax.broadcasted_iota(jnp.int32, (2 * lanes, lanes), 0) & (lanes - 1)
    col = lax.broadcasted_iota(jnp.int32, (2 * lanes, lanes), 1)
    half = dirs * channels
    same = ((row >= half) == (col >= half)) & ((row & (channels - 1)) == (col & (channels - 1)))
    mixer[...] = jnp.where(same, -1.0, 0.0).astype(jnp.bfloat16)

    def window(first, second, i):
        offset = (2 * width * i) % 128
        if offset == 0:
            return first
        back = 128 - offset
        lane = lax.broadcasted_iota(jnp.int32, first.shape, 1)
        return jnp.where(lane < back, pltpu.roll(first, back, 1), pltpu.roll(second, back, 1))

    def swung(left, right):
        return lax.dot_general(left, right, (((1,), (1,)), ((), ())), preferred_element_type=jnp.float32)

    loads[0].wait()
    for part in range(2):
        for pol in range(pols):
            for f in range(channels):
                vis_rows[part, pol * channels + f : pol * channels + f + 1, 0:pairs] = vis_raw[part, pol, f]
    upper = lax.broadcasted_iota(jnp.int32, (2 * channels, 128), 0) < channels
    lane = lax.broadcasted_iota(jnp.int32, (2 * PITCH, lanes), 1)
    real = (lane & 8) == 0
    gap = jnp.zeros((half - 16, 128), jnp.float32)

    def vis_side(i):
        j = (2 * width * i) // 128
        first, second = [], []
        for part in range(2):
            value = window(vis_rows[part, :, 128 * j : 128 * j + 128], vis_rows[part, :, 128 * j + 128 : 128 * j + 256], i)
            high = value.astype(jnp.bfloat16).astype(jnp.float32)
            low = pltpu.roll(value - high, channels, 0)
            first.append(jnp.where(upper, high, low))
            second.append(jnp.where(upper, low, high))
        return jnp.concatenate(first + [gap] + second + [gap], 0).astype(jnp.bfloat16)

    for i in range(0, width // 2, 2):
        both = range(i, min(i + 2, width // 2))
        turned = swung(chooser[...], jnp.concatenate([vis_side(k) for k in both], 0))
        for n, k in enumerate(both):
            mine = turned[:, n * lanes : (n + 1) * lanes]
            vis[0, 2 * k : 2 * k + 2] = jnp.where(real, mine, 0.0).reshape(2, PITCH, lanes)
            vis[1, 2 * k : 2 * k + 2] = jnp.where(real, 0.0, mine).reshape(2, PITCH, lanes)

    for copy in loads[1:]:
        copy.wait()
    for part in range(2):
        start = jnp.transpose(jones_raw[part].reshape(lanes, width))
        gain[0, part, 0:width] = start
        cons[part, 0:width] = start
        dual[part, 0:width] = jnp.transpose(duals_raw[part].reshape(lanes, width))
        empty = jnp.zeros((PITCH - width, lanes), jnp.float32)
        gain[0, part, width:] = empty
        cons[part, width:] = empty
        dual[part, width:] = empty

    state = {"tile": 0, "left": None, "have": 0}

    def fetched(limit):
        while state["have"] < min(limit, tiles):
            if state["have"] < whole:
                sky_loads[state["have"]].wait()
            else:
                tail_load.wait()
                sky_raw[whole, :, :, :, 0 : pairs - 128 * whole] = tail_raw[...]
            state["have"] += 1

    flat = sky.reshape(2, PITCH * PITCH, lanes)

    def turn(limit):
        while state["tile"] < tiles and bases[state["tile"]] < limit:
            j = state["tile"]
            turned = swung(placer[j], sky_raw[j].reshape(2 * lanes, 128))
            size = bases[j + 1] - bases[j]
            left = []
            for part in range(2):
                mine = turned[:, part * lanes : (part + 1) * lanes]
                head = mine[0:8]
                if state["left"] is not None:
                    head = head + state["left"][part]
                flat[part, bases[j] : bases[j] + 8] = head
                if size > 8:
                    flat[part, bases[j] + 8 : bases[j + 1]] = mine[8:size]
                left.append(mine[size : size + 8] if size + 8 <= TALL else None)
            state["tile"], state["left"] = j + 1, left

    def parted(value):
        high = value.astype(jnp.bfloat16)
        low = (value - high.astype(jnp.float32)).astype(jnp.bfloat16)
        return jnp.concatenate([high, low], 1)

    def gathered_rows(values):
        row = lax.broadcasted_iota(jnp.int32, (8, lanes), 0)
        for bit in (1, 2, 4):
            even = (row & bit) == 0
            values = [
                jnp.where(even, a, b) + pltpu.roll(jnp.where(even, b, a), bit, 0)
                for a, b in zip(values[0::2], values[1::2])
            ]
        return values[0]

    def front(it, block):
        gr, gi = gain[it, 0], gain[it, 1]
        bank = block % 2
        sides = ([], [])
        here = min(GROUP, width - block * GROUP)
        for b in range(here):
            p = block * GROUP + b
            sr, si = sky[0, p], sky[1, p]
            zr = sr * gr + si * gi
            zi = sr * gi - si * gr
            z_keep[bank, 0, b] = zr
            z_keep[bank, 1, b] = zi
            lr, li = gain[it, 0, p : p + 1], gain[it, 1, p : p + 1]
            sides[0].append(parted(lr * zr + li * zi - vis[0, p]))
            sides[1].append(parted(li * zr - lr * zi - vis[1, p]))
        for part in range(2):
            rest[bank, part, 0:here] = jnp.dot(
                jnp.concatenate(sides[part], 0), mixer[...], preferred_element_type=jnp.float32
            ).reshape(here, PITCH, lanes)

    def back(block):
        bank = block % 2
        sums_of = [[], [], []]
        for b in range(min(GROUP, width - block * GROUP)):
            zr, zi = z_keep[bank, 0, b], z_keep[bank, 1, b]
            dr, di = rest[bank, 0, b], rest[bank, 1, b]
            for i, value in enumerate((dr * zr - di * zi, dr * zi + di * zr, zr * zr + zi * zi)):
                sums_of[i].append(jnp.sum(value.reshape(PITCH // 8, 8, lanes), 0))
        for i in range(3):
            sums_of[i] += [jnp.zeros((8, lanes), jnp.float32)] * (GROUP - len(sums_of[i]))
            acc[i, block * GROUP : (block + 1) * GROUP] = gathered_rows(sums_of[i])

    place = lax.broadcasted_iota(jnp.int32, (8, lanes), 1) & (channels - 1)

    def mixed(block, distance):
        out = None
        for shift in range(1 - channels, channels):
            offset = distance + shift + 4
            if offset < 0 or offset > 8:
                continue
            inside = (place + shift >= 0) & (place + shift < channels)
            weight = jnp.where(inside, kernel_taps[offset], 0.0)[0:1]
            moved = block if shift == 0 else pltpu.roll(block, (-shift) % lanes, 1)
            term = weight * moved
            out = term if out is None else out + term
        return out

    def up_copy(it, chunk):
        return pltpu.make_async_remote_copy(
            src_ref=summed.at[it, :, slice(*CHUNKS[chunk])], dst_ref=from_low.at[it, :, slice(*CHUNKS[chunk])],
            send_sem=send_sem.at[it, chunk, 0], recv_sem=low_sem.at[it, chunk],
            device_id={"chan": lax.rem(me + 1, count)}, device_id_type=MESH,
        )

    def down_copy(it, chunk):
        return pltpu.make_async_remote_copy(
            src_ref=summed.at[it, :, slice(*CHUNKS[chunk])], dst_ref=from_high.at[it, :, slice(*CHUNKS[chunk])],
            send_sem=send_sem.at[it, chunk, 1], recv_sem=high_sem.at[it, chunk],
            device_id={"chan": lax.rem(me + count - 1, count)}, device_id_type=MESH,
        )

    def finish(it, chunk):
        rows = slice(*CHUNKS[chunk])
        lower = acc[2, rows]
        scale = 1.0 / (lower + penalty)
        for part in range(2):
            goal = cons[part, rows] - dual[part, rows]
            fresh = (acc[part, rows] + gain[it, part, rows] * lower + penalty * goal) * scale
            gain[it + 1, part, rows] = fresh
            summed[it, part, rows] = fresh + dual[part, rows]

        @pl.when(me < count - 1)
        def _():
            up_copy(it, chunk).start()

        @pl.when(me > 0)
        def _():
            down_copy(it, chunk).start()

    def smooth(it, chunk):
        rows = slice(*CHUNKS[chunk])
        own = [mixed(summed[it, part, rows], 0) for part in range(2)]

        @pl.when(me > 0)
        def _():
            up_copy(it, chunk).wait_recv()

        @pl.when(me < count - 1)
        def _():
            down_copy(it, chunk).wait_recv()

        for part in range(2):
            fresh = (
                own[part]
                + mixed(from_low[it, part, rows], -channels)
                + mixed(from_high[it, part, rows], channels)
            )
            off = gain[it + 1, part, rows] - fresh
            moved = fresh - cons[part, rows]
            dual[part, rows] = dual[part, rows] + off
            cons[part, rows] = fresh
            sums[2 * it] += jnp.sum((off * off).reshape(-1, 8, lanes), 0)
            sums[2 * it + 1] += jnp.sum((moved * moved).reshape(-1, 8, lanes), 0)

    def norm_copy(step):
        return pltpu.make_async_remote_copy(
            src_ref=partial, dst_ref=slots.at[me],
            send_sem=norm_send.at[step], recv_sem=norm_recv.at[step],
            device_id={"chan": lax.rem(me + step, count)}, device_id_type=MESH,
        )

    def put(target, state):
        for part in range(2):
            target[part] = jnp.transpose(state[part])[:, 0:width].reshape(pols, dirs, channels, width)

    blocks = PITCH // GROUP
    stops = {stop // GROUP - 1: chunk for chunk, (_, stop) in enumerate(CHUNKS)}
    fetched(10)
    turn(2 * GROUP * PITCH)
    fetched(tiles)
    for it in range(ITERS):
        front(it, 0)
        for block in range(blocks):
            if it == 0:
                turn((block + 2) * GROUP * PITCH)
            if block + 1 < blocks:
                front(it, block + 1)
            back(block)
            if it == 0 and block in stops:
                if stops[block] == 0:
                    pl.semaphore_wait(barrier, count - 1)
                finish(it, stops[block])
            if it > 0:
                for chunk, hold in enumerate(HOLDS):
                    if block == hold:
                        smooth(it - 1, chunk)
                        finish(it, chunk)
    for chunk in range(len(CHUNKS)):
        smooth(ITERS - 1, chunk)

    lane = lax.broadcasted_iota(jnp.int32, (1, lanes), 1)
    share = lanes // (2 * ITERS)
    packed = jnp.zeros((1, lanes), jnp.float32)
    for i in range(2 * ITERS):
        value = jnp.sum(sums[i], 0, keepdims=True)
        stride = lanes // 2
        while stride >= share:
            value = value + pltpu.roll(value, stride, 1)
            stride //= 2
        packed = jnp.where(lane // share == i, value, packed)
    partial[...] = packed
    slots[pl.ds(me, 1)] = packed[None]
    for step in range(1, count):
        norm_copy(step).start()
    put(jones_out, gain.at[ITERS])
    put(consensus_out, cons)
    put(duals_out, dual)

    for it in range(ITERS):
        for chunk in range(len(CHUNKS)):

            @pl.when(me < count - 1)
            def _():
                up_copy(it, chunk).wait_send()

            @pl.when(me > 0)
            def _():
                down_copy(it, chunk).wait_send()

    for step in range(1, count):
        norm_copy(step).wait_send()
    for step in range(1, count):
        norm_copy(step).wait_recv()
    gathered = slots[0]
    for j in range(1, count):
        gathered = gathered + slots[j]
    for it in range(ITERS):
        for n, factor in enumerate((1.0, penalty * penalty)):
            mine = jnp.where(lane // share == 2 * it + n, gathered, 0.0)
            norms_out[it : it + 1, n : n + 1] = jnp.sum(mine, axis=1, keepdims=True) * (factor / entries)


def deliver(*refs):
    sources, targets, sem = refs[0:4], refs[4:8], refs[8]
    copies = [pltpu.make_async_copy(s, t, sem.at[i]) for i, (s, t) in enumerate(zip(sources, targets))]
    for copy in copies:
        copy.start()
    for copy in copies:
        copy.wait()


def solution(mesh):
    count = mesh.shape["chan"]

    def local(visibility, coherency, jones_start, duals_start):
        _, pols, dirs, channels, width = jones_start.shape
        pairs = visibility.shape[-1]
        times = visibility.shape[3]
        lanes = pols * dirs * channels
        assert times == 1 and pols == 2 and channels == 4 and lanes == 128 and width <= PITCH - 2 and width % 2 == 0
        tiles = pl.cdiv(pairs, 128)
        whole = pairs // 128
        entries = jones_start.size * count
        sky = coherency.transpose(0, 1, 2, 4, 3, 5).reshape(2, pols, dirs, channels, pairs)
        state = jax.ShapeDtypeStruct(jones_start.shape, jnp.float32)
        f32, bf16 = jnp.float32, jnp.bfloat16
        shapes = (state, state, state, jax.ShapeDtypeStruct((ITERS, 2), f32))
        packed = (2, PITCH, lanes)
        halo = (ITERS, 2, PITCH, lanes)
        parts = len(CHUNKS)
        results = pl.pallas_call(
            functools.partial(kernel, count, (pols, dirs, channels, width, pairs, entries)),
            out_shape=shapes,
            in_specs=[pl.BlockSpec(memory_space=pl.ANY)] * 4,
            out_specs=tuple([pl.BlockSpec(memory_space=pltpu.VMEM)] * 4),
            scratch_shapes=[
                pltpu.VMEM(visibility.shape, f32),
                pltpu.VMEM((tiles, 2, pols, dirs * channels, 128), bf16),
                pltpu.VMEM((2, pols, dirs * channels, pairs - 128 * whole), bf16),
                pltpu.VMEM(jones_start.shape, f32),
                pltpu.VMEM(duals_start.shape, f32),
                pltpu.VMEM((2, 2 * channels, tiles * 128), f32),
                pltpu.VMEM((2 * PITCH, 128), bf16),
                pltpu.VMEM((tiles, TALL, 128), bf16),
                pltpu.VMEM((2 * lanes, lanes), bf16),
                pltpu.VMEM((2, PITCH, PITCH, lanes), f32),
                pltpu.VMEM((2, PITCH, PITCH, lanes), f32),
                pltpu.VMEM((2, 2, GROUP, PITCH, lanes), f32),
                pltpu.VMEM((2, 2, GROUP, PITCH, lanes), f32),
                pltpu.VMEM((3, PITCH, lanes), f32),
                pltpu.VMEM((ITERS + 1,) + packed, f32),
                pltpu.VMEM(packed, f32),
                pltpu.VMEM(packed, f32),
                pltpu.VMEM(halo, f32),
                pltpu.VMEM(halo, f32),
                pltpu.VMEM(halo, f32),
                pltpu.VMEM((2 * ITERS, 8, lanes), f32),
                pltpu.VMEM((1, lanes), f32),
                pltpu.VMEM((count, 1, lanes), f32),
                pltpu.SemaphoreType.DMA((3,)),
                pltpu.SemaphoreType.DMA((whole,)),
                pltpu.SemaphoreType.DMA,
                pltpu.SemaphoreType.DMA((ITERS, parts, 2)),
                pltpu.SemaphoreType.DMA((ITERS, parts)),
                pltpu.SemaphoreType.DMA((ITERS, parts)),
                pltpu.SemaphoreType.DMA((count,)),
                pltpu.SemaphoreType.DMA((count,)),
            ],
            compiler_params=pltpu.CompilerParams(
                collective_id=0, has_side_effects=True, vmem_limit_bytes=24 * 1024 * 1024
            ),
        )(*[pltpu.with_memory_space_constraint(x, pltpu.HBM) for x in (visibility, sky, jones_start, duals_start)])
        return pl.pallas_call(
            deliver,
            out_shape=shapes,
            in_specs=[pl.BlockSpec(memory_space=pltpu.VMEM)] * 4,
            out_specs=tuple([pl.BlockSpec(memory_space=pl.ANY)] * 4),
            scratch_shapes=[pltpu.SemaphoreType.DMA((4,))],
            compiler_params=pltpu.CompilerParams(vmem_limit_bytes=4 * 1024 * 1024),
        )(*results)

    placed = (
        P(None, None, "chan", "slot", None),
        P(None, None, None, "chan", "slot", None),
        P(None, None, "slot", "chan", None),
        P(None, None, "slot", "chan", None),
    )
    return jax.shard_map(
        local,
        mesh=mesh,
        in_specs=placed,
        out_specs=(
            P(None, None, "slot", "chan", None),
            P(None, None, "slot", "chan", None),
            P(None, None, "slot", "chan", None),
            P("slot", None),
        ),
        check_vma=False,
    )
```
